128 devices in a mesh: gx: 4 (over x), gy: 4 (over z), gz: 8 (over y, core).
Axes of the slice: x: 4, y: 4, z: 4, core: 2. Of those that a mesh axis runs over, the one named last changes fastest.
Arguments:
- coords: float32 [4, 4, 24, 3, 128], P('gx', 'gy', 'gz'), as said below
- polar: float32 [4, 4, 24, 128], P('gx', 'gy', 'gz'), may hold values from 0.3 to 1.2
- field: float32 [4, 4, 24, 6, 128], P('gx', 'gy', 'gz'), may hold values from -6 to 6
- atom_count: int32 [4, 4, 24], P('gx', 'gy', 'gz'), may hold values from 64 to 128, as said below
- pair_list: int32 [4, 4, 24, 13], P('gx', 'gy', 'gz'), may hold values from -1 to 26, as said below
Outputs:
- dipoles: float32 [4, 4, 24, 6, 128], P('gx', 'gy', 'gz')
- residual: float32 [4, 4, 24, 6, 128], P('gx', 'gy', 'gz')
The draws below stay inside these ranges and needn't reach their ends.
Inputs may be any that keep to these rules, and one draw needn't show every extreme that they name: `coords`: each coordinate lies within a quarter of 2.2 of its lattice site: atom slot a sits at 2.2 (a % 4 + 0.5, (a // 4) % 4 + 0.5, a // 16 + 0.5). `atom_count`: some block holds 128 atoms. `pair_list`: each block's row holds distinct codes above 13 in ascending order, followed by -1 in the unused entries.
All inputs are finite; a program needn't handle non-finite values.
Results may differ from the reference program's by a relative error of at most 0.0003.
Values sent between devices are 32-bit elements; how exact they have to be, the bound alone decides.
A program may use at most 64 MiB of HBM per device.

```python
import math
import jax
import jax.numpy as jnp
from jax import lax

ATOMS = 128
ITERS = 2
NBX = 4
NBY = 4
NBZ = 24


spacing = 2.2


def draw_coords(key, part):
    lattice_ids = jnp.arange(ATOMS, dtype=jnp.int32)
    lattice = jnp.stack([lattice_ids % 4, lattice_ids // 4 % 4, lattice_ids // 16]).astype(jnp.float32)
    lattice_pos = (lattice + 0.5) * spacing
    jitter = jax.random.uniform(key, (NBX, NBY, NBZ, 3, ATOMS), jnp.float32, -0.2, 0.2)
    return (lattice_pos + jitter * spacing).astype(jnp.float32)


def draw_atom_count(key, part):
    counts = jax.random.randint(key, (NBX, NBY, NBZ), ATOMS // 2, ATOMS + 1)
    return counts.at[0, 0, 0].set(ATOMS).astype(jnp.int32)


def draw_pair_list(key, part):
    dice_rolls = jax.random.randint(key, (NBX, NBY, NBZ, 13), 0, 100)
    density = jnp.arange(NBX, dtype=jnp.int32) * 60 // NBX + 30
    chosen = dice_rolls < density[:, None, None, None]
    forward_codes = jnp.arange(14, 27, dtype=jnp.int32)
    sort_keys = jnp.where(chosen, forward_codes, forward_codes + 100)
    ordered = jnp.sort(sort_keys, axis=-1)
    return jnp.where(ordered < 100, ordered, -1).astype(jnp.int32)


def shard_levels(stream_key, extent, pieces, least, top_value):
    def one(position, parts):
        draws = jax.random.uniform(jax.random.fold_in(jax.random.fold_in(stream_key, 6), position), (parts,), jnp.float32, least / len(pieces), top_value / len(pieces))
        return jnp.repeat(jnp.exp(draws), extent[position] // parts).reshape((-1,) + (1,) * (len(extent) - position - 1))

    gain = one(*pieces[0])
    for cut in pieces[1:]:
        gain = gain * one(*cut)
    return gain


def noise(rng, shape, scale, bound, split=(), held_as=jnp.bfloat16):
    result = jax.random.normal(rng, shape, jnp.float32) * scale
    if len(split) > 0:
        result = shard_levels(rng, shape, split, -0.22, 0.18) * result
    return jnp.clip(result, min=-bound, max=bound).astype(held_as)


def setup_inputs(seed: int = 0) -> dict:
    seeds = jax.random.split(jax.random.key(seed), 6)
    return {
        "coords": draw_coords(jax.random.fold_in(seeds[5], 71), 0),
        "polar": jnp.clip(jnp.exp(math.log(1.2) - 1.3862944 * jax.random.uniform(seeds[1], (NBX, NBY, NBZ, ATOMS), jnp.float32) ** shard_levels(seeds[1], (NBX, NBY, NBZ, ATOMS), ((0, 4), (1, 4), (2, 8)), -0.2, 0.2)), 0.3, 1.2),
        "field": noise(seeds[2], (NBX, NBY, NBZ, 6, ATOMS), 1.0, 6.0, ((0, 4), (1, 4), (2, 8)), jnp.float32),
        "atom_count": draw_atom_count(jax.random.fold_in(seeds[5], 71), 0),
        "pair_list": draw_pair_list(jax.random.fold_in(seeds[5], 71), 0),
    }


spacing = 2.2
cutoff_square = 49.0
thole = 0.39
highest = lax.Precision.HIGHEST

def pair_weights(geometry_row, geometry_col, offset_vec, self_flag):
    separation = offset_vec[:, None, None] + geometry_col[0:3][:, None, :] - geometry_row[0:3][:, :, None]
    range_square = lax.optimization_barrier(jnp.sum(separation * separation, axis=0))
    diagonal = self_flag * jnp.eye(geometry_row.shape[1], dtype=jnp.float32)
    weight_mask = geometry_row[4][:, None] * geometry_col[4][None, :] * (1.0 - diagonal)
    range_square = range_square + diagonal
    inverse_range = lax.rsqrt(range_square)
    inverse_cube = inverse_range * inverse_range * inverse_range
    damp_argument = thole * range_square * jnp.sqrt(range_square) * lax.rsqrt(geometry_row[3][:, None] * geometry_col[3][None, :])
    damping = jnp.exp(-damp_argument)
    lam_three = 1.0 - damping
    lam_five = 1.0 - (1.0 + damp_argument) * damping
    switch = jnp.square(jnp.maximum(1.0 - range_square / cutoff_square, 0.0))
    weight_three = weight_mask * switch * lam_three * inverse_cube
    weight_five = 3.0 * weight_mask * switch * lam_five * inverse_cube * inverse_range * inverse_range
    return (weight_three, weight_five, separation)

def field_rows(weight_three, weight_five, separation, dipole_col):
    dipole_sets = dipole_col.reshape(2, 3, -1)
    projected = jnp.einsum('cij,scj->sij', separation, dipole_sets, precision=highest)
    radial = jnp.einsum('ij,cij,sij->sci', weight_five, separation, projected, precision=highest)
    direct = jnp.einsum('ij,scj->sci', weight_three, dipole_sets, precision=highest)
    return (radial - direct).reshape(6, -1)

def block_fields(geometry, neighbour_geo, neighbour_dip, active, offset_vec, self_flag):

    def slab_fields(inputs):
        geo_slab, near_geo, near_dip, act_slab = inputs
        atom_slots = geo_slab.shape[-1]

        def single_pair(geometry_row, geometry_col, dipole_col, switch_on):
            weight_three, weight_five, separation = pair_weights(geometry_row, geometry_col, offset_vec, self_flag)
            return switch_on * field_rows(weight_three, weight_five, separation, dipole_col)
        fields = jax.vmap(single_pair)(geo_slab.reshape(-1, 5, atom_slots), near_geo.reshape(-1, 5, atom_slots), near_dip.reshape(-1, 6, atom_slots), act_slab.reshape(-1))
        return fields.reshape(geo_slab.shape[0:2] + (6, atom_slots))
    return lax.map(slab_fields, (geometry, neighbour_geo, neighbour_dip, active))

def apply_operator(vector, geometry, forward, box_size):
    accumulated = jnp.zeros_like(vector)
    for pair_code in range(27):
        roll_by = (1 - pair_code // 9, 1 - pair_code // 3 % 3, 1 - pair_code % 3)
        neighbour_geo = jnp.roll(geometry, roll_by, axis=(0, 1, 2))
        neighbour_dip = jnp.roll(vector, roll_by, axis=(0, 1, 2))
        if pair_code == 13:
            active = jnp.ones(forward.shape[0:3], jnp.float32)
        elif pair_code > 13:
            active = forward[..., pair_code]
        else:
            active = jnp.roll(forward[..., 26 - pair_code], roll_by, axis=(0, 1, 2))
        offset_vec = box_size * jnp.array([pair_code // 9 - 1, pair_code // 3 % 3 - 1, pair_code % 3 - 1], jnp.float32)
        self_flag = 1.0 if pair_code == 13 else 0.0
        accumulated = accumulated + block_fields(geometry, neighbour_geo, neighbour_dip, active, offset_vec, self_flag)
    return vector / geometry[:, :, :, 3:4, :] - accumulated

def set_sums(former, latter):
    product = (former * latter).reshape(former.shape[0:3] + (2, 3, former.shape[-1]))
    return lax.optimization_barrier(jnp.sum(product, axis=(0, 1, 2, 4, 5)))

def spread(values):
    return jnp.repeat(values, 3)[:, None]

def reference(coords, polar, field, atom_count, pair_list):
    atom_slots = coords.shape[-1]
    slot_ids = jnp.arange(atom_slots, dtype=jnp.int32)
    atom_mask = (slot_ids[None, None, None, :] < atom_count[..., None]).astype(jnp.float32)
    geometry = jnp.concatenate([coords, polar[..., None, :], atom_mask[..., None, :]], axis=3)
    pair_codes = jnp.arange(27, dtype=jnp.int32)
    forward = jnp.any(pair_list[..., :, None] == pair_codes, axis=-2).astype(jnp.float32)
    box_size = jnp.array([4.0 * spacing, 4.0 * spacing, spacing * (atom_slots // 16)], jnp.float32)
    polar_col = geometry[:, :, :, 3:4, :]
    source = field * atom_mask[..., None, :]
    dipoles = polar_col * source
    residual = source - apply_operator(dipoles, geometry, forward, box_size)
    precond = polar_col * residual
    direction = precond
    norm_now = set_sums(residual, precond)
    for iteration in range(ITERS):
        operated = apply_operator(direction, geometry, forward, box_size)
        step_len = spread(norm_now / set_sums(direction, operated))
        dipoles = dipoles + step_len * direction
        residual = residual - step_len * operated
        if iteration + 1 < ITERS:
            precond = polar_col * residual
            norm_next = set_sums(residual, precond)
            direction = precond + spread(norm_next / norm_now) * direction
            norm_now = norm_next
    return (dipoles, residual)
```

```python
import functools

import jax
import jax.numpy as jnp
from jax import lax
from jax.experimental import pallas as pl
from jax.experimental.pallas import tpu as pltpu
from jax.sharding import PartitionSpec as P


F32 = jnp.float32
I32 = jnp.int32
MESH = pl.DeviceIdType.MESH
SPACING = 2.2
HIGH = 2.1875
LOW = 0.0125
CUT2 = 49.0
THOLE = 0.39
SIZES = {"gx": 4, "gy": 4, "gz": 8}

NEAR = [(ox, oy, oz) for ox in (-1, 0, 1) for oy in (-1, 0, 1) for oz in (-1, 0, 1) if (ox, oy, oz) != (0, 0, 0)]
NEAR_ID = {n: i for i, n in enumerate(NEAR)}
FLAT = [n for n in NEAR if n[2] == 0]
FLAT_ID = {n: i for i, n in enumerate(FLAT)}
EDGE = [n for n in NEAR if n[2] != 0]
EDGE_ID = {n: i for i, n in enumerate(EDGE)}
PLANE = [(i, j) for i in range(4) for j in range(4)]
GREETED = sorted(
    {(ox % 4, oy % 4, oz % 8) for ox, oy, oz in NEAR}
    | {(i, j, 0) for i, j in PLANE if (i, j) != (0, 0)}
    | {(0, 0, k) for k in range(1, 8)}
)

OWN_COLS = [3, 4, 5, 6]
FAR_COLS = [0, 1, 2, 7, 8, 9]
OWN_PAIRS = [(x, c) for c in OWN_COLS for x in range(4)]
FAR_PAIRS = [(x, c) for c in FAR_COLS for x in range(4) if abs(c - 3 - x) <= 3]


def col_home(col):
    return (-1, col + 1) if col < 3 else (0, col - 3) if col < 7 else (1, col - 7)


def lanes():
    return lax.broadcasted_iota(I32, (8, 128), 1)


def subs():
    return lax.broadcasted_iota(I32, (8, 128), 0)


def row_of(ref, *where):
    return jnp.broadcast_to(ref[where], (8, 128))


def kernel(
    coords, polar, field, count, pairs, dip_out, res_out,
    packed, first, first_edge, vec, vec_edge, src, pol, ipol, own_geo,
    in_first, in_first_edge, in_vec, in_vec_edge, ext, merged, geo, act, dip, tens, acc, rows,
    part, in_plane, part2, in_line,
    send_sem, recv_sem, plane_send, plane_recv, line_send, line_recv,
):
    me = {a: lax.axis_index(a) for a in SIZES}

    def at(ox, oy, oz):
        off = {"gx": ox, "gy": oy, "gz": oz}
        return {a: lax.rem(me[a] + off[a] % SIZES[a], SIZES[a]) for a in SIZES}

    barrier = pltpu.get_barrier_semaphore()
    for ox, oy, oz in GREETED:
        pl.semaphore_signal(barrier, inc=1, device_id=at(ox, oy, oz), device_id_type=MESH)

    lane, sub = lanes(), subs()
    l32 = lane & 31
    zz = l32 - 3
    group = lane >> 5
    blk = zz >> 3
    valid = (zz >= 0) & (zz < 24)
    dz = 3 - sub

    for b in range(3):
        slot = lane
        mask = (slot[0:1] < count[0, 0, b]).astype(F32)
        packed[b, 0] = jnp.zeros((8, 128), F32)
        packed[b, 1] = jnp.zeros((8, 128), F32)
        packed[b, 0, 0:6, :] = field[0, 0, b] * mask
        pol_row = polar[0, 0, b : b + 1, :]
        packed[b, 0, 6:7, :] = pol_row
        s3 = slot[0:3]
        r3 = sub[0:3]
        site = jnp.where(r3 == 0, s3 & 3, jnp.where(r3 == 1, (s3 >> 2) & 3, s3 >> 4)).astype(F32) + 0.5
        packed[b, 1, 0:3, :] = (coords[0, 0, b] - site * HIGH) - site * LOW
        packed[b, 1, 3:4, :] = mask * lax.rsqrt(pol_row)
    bits = []
    for b in range(3):
        word = jnp.int32(0)
        for k in range(13):
            word = word | (jnp.int32(1) << (pairs[0, 0, b, k] & 31))
        bits.append(word)
    word = jnp.where(blk <= 0, bits[0], jnp.where(blk == 1, bits[1], bits[2]))
    for x in range(4):
        pick = 16 * (zz & 7) + 4 * group + x
        tile = []
        for t in range(2):
            got = [jnp.take_along_axis(packed[b, t], pick, axis=1) for b in range(3)]
            tile.append(jnp.where(valid, jnp.where(blk == 0, got[0], jnp.where(blk == 1, got[1], got[2])), 0.0))
        code = jnp.where(sub == 7, 14, jnp.maximum(15 + 3 * x + sub - 4, 0))
        flag = (lax.shift_right_logical(word, code) & 1).astype(F32)
        first[x, 0:8, :] = jnp.where((sub >= 4) & valid, flag, tile[1])
        src[x] = jnp.where(sub < 6, tile[0], 0.0)
        rows[x] = jnp.where((sub == 6) & valid, tile[0], 1.0)
        p = row_of(rows, x, slice(6, 7))
        pol[x] = p
        ipol[x] = 1.0 / p
        first[x, 8:16, :] = src[x] * p

    def edge_of(tiles):
        out = jnp.zeros((8, 128), F32)
        for x in range(4):
            top = pltpu.roll(tiles[x], (8 * x - 24) % 128, 1)
            low = pltpu.roll(tiles[x], (8 * x + 1) % 128, 1)
            out = jnp.where((l32 >= 8 * x) & (l32 < 8 * x + 3), top, out)
            out = jnp.where((l32 >= 8 * x + 4) & (l32 < 8 * x + 7), low, out)
        return out

    first_edge[0:8, :] = edge_of([first[x, 0:8, :] for x in range(4)])
    first_edge[8:16, :] = edge_of([first[x, 8:16, :] for x in range(4)])

    pl.semaphore_wait(barrier, len(GREETED))

    def copy(phase, n, incoming):
        ox, oy, oz = n if not incoming else tuple(-v for v in n)
        back = (-ox, -oy, -oz)
        count_rows = 14 if phase == 0 else 6
        if oz == 0:
            lo, hi = (1, 4) if ox == 1 else (0, 3) if ox == -1 else (0, 4)
            if phase == 0:
                s, d = first, in_first.at[FLAT_ID[back]]
            else:
                s, d = vec.at[phase - 1], in_vec.at[phase - 1, FLAT_ID[back]]
            s, d = s.at[lo:hi, 0:count_rows, :], d.at[lo:hi, 0:count_rows, :]
        else:
            if phase == 0:
                s, d = first_edge, in_first_edge.at[EDGE_ID[back]]
            else:
                s, d = vec_edge.at[phase - 1], in_vec_edge.at[phase - 1, EDGE_ID[back]]
            s, d = s.at[0:count_rows, :], d.at[0:count_rows, :]
        return pltpu.make_async_remote_copy(
            src_ref=s, dst_ref=d,
            send_sem=send_sem.at[phase, NEAR_ID[(ox, oy, oz)]], recv_sem=recv_sem.at[phase, NEAR_ID[back]],
            device_id=at(ox, oy, oz), device_id_type=MESH,
        )

    ORDER = sorted(NEAR, key=lambda n: (n[0] == 0, -sum(map(abs, n))))

    def send(phase):
        for n in sorted(NEAR, key=lambda n: (n[2] != 0, -sum(map(abs, n)))):
            copy(phase, n, False).start()

    def await_near(phase, far):
        for n in ORDER:
            if (n[0] != 0) == far:
                copy(phase, n, True).wait_recv()

    def ext_tile(phase, r0, ox, oy, x):
        if phase == 0:
            here = first[x, r0 : r0 + 8, :] if (ox, oy) == (0, 0) else in_first[FLAT_ID[(ox, oy, 0)], x, r0 : r0 + 8, :]
            low = in_first_edge[EDGE_ID[(ox, oy, -1)], r0 : r0 + 8, :]
            top = in_first_edge[EDGE_ID[(ox, oy, 1)], r0 : r0 + 8, :]
        else:
            here = vec[phase - 1, x] if (ox, oy) == (0, 0) else in_vec[phase - 1, FLAT_ID[(ox, oy, 0)], x]
            low = in_vec_edge[phase - 1, EDGE_ID[(ox, oy, -1)]]
            top = in_vec_edge[phase - 1, EDGE_ID[(ox, oy, 1)]]
        low = pltpu.roll(low, (-8 * x) % 128, 1)
        top = pltpu.roll(top, (23 - 8 * x) % 128, 1)
        return jnp.where(l32 < 3, low, jnp.where(l32 >= 27, top, here))

    def slide(ref, where, shift):
        return pltpu.roll(row_of(ref, *where), shift % 128, 1, stride=1, stride_axis=0)

    def merge_column(phase, r0, col):
        ox, x = col_home(col)
        tiles = {oy: ext_tile(phase, r0, ox, oy, x) for oy in (-1, 0, 1)}
        for k in range(7):
            dy = k - 3
            if dy > 0:
                tile = jnp.where(group < dy, tiles[1], tiles[0])
            elif dy < 0:
                tile = jnp.where(group >= 4 + dy, tiles[-1], tiles[0])
            else:
                tile = pltpu.roll(tiles[0], 64, 1)
            merged[col, k] = tile
        return tiles

    def merged_shift(k):
        return -32 * (k - 3) - 3 - (64 if k == 3 else 0)

    def spread_dipoles(phase, cols):
        for col in cols:
            merge_column(phase, 8 if phase == 0 else 0, col)
        for col in cols:
            for k in range(7):
                for c in range(6):
                    dip[col, k, c] = slide(merged, (col, k, slice(c, c + 1)), merged_shift(k))

    zp = zz + dz
    oz = (lax.shift_right_arithmetic(zp + 8, 3)) - (lax.shift_right_arithmetic(zz + 8, 3))
    lawful = valid & (sub < 7)

    def forward_act(ox, oy):
        x = 0 if ox == 0 else 2 + oy
        k = [row_of(first, x, slice(4 + i, 5 + i)) for i in range(3)]
        return jnp.where(oz == 0, k[1], jnp.where(oz > 0, k[2], k[0]))

    def backward_act(ox, oy):
        x = 0 if ox == 0 else 2 - oy
        ext[0] = ext_tile(0, 0, ox, oy, x)
        k = [slide(ext, (0, slice(4 + i, 5 + i)), -35) for i in range(3)]
        return jnp.where(oz == 0, k[1], jnp.where(oz > 0, k[0], k[2]))

    def self_act():
        ext[0] = ext_tile(0, 0, 0, 0, 0)
        up = row_of(first, 0, slice(7, 8))
        down = slide(ext, (0, slice(7, 8)), -35)
        return jnp.where(oz == 0, 1.0, jnp.where(oz > 0, up, down))

    def acts(ox):
        if ox == 0:
            a = {-1: backward_act(0, -1), 0: self_act(), 1: forward_act(0, 1)}
        else:
            a = {oy: (forward_act if ox > 0 else backward_act)(ox, oy) for oy in (-1, 0, 1)}
        for k in range(7):
            to = group + (k - 3)
            tile = jnp.where(to < 0, a[-1], jnp.where(to > 3, a[1], a[0]))
            act[ox + 1, k] = jnp.where(lawful, tile, 0.0)

    def spread_geometry(cols):
        for ox in sorted({col_home(c)[0] for c in cols}):
            acts(ox)
        for col in cols:
            merge_column(0, 0, col)
        for col in cols:
            ox, x = col_home(col)
            for k in range(7):
                for c in range(4):
                    tile = slide(merged, (col, k, slice(c, c + 1)), merged_shift(k))
                    if c == 2:
                        tile = tile + SPACING * dz.astype(F32)
                    if c == 3:
                        tile = tile * act[ox + 1, k]
                    geo[col, k, c] = tile

    def tensors(pair_list, base):
        def body(k, carry):
            shift_y = SPACING * (k - 3).astype(F32)
            for i, (x, col) in enumerate(pair_list):
                off_x = col - 3 - x
                dx = geo[col, k, 0] - own_geo[x, 0]
                if off_x:
                    dx = dx + SPACING * off_x
                dy = geo[col, k, 1] - own_geo[x, 1] + shift_y
                dzz = geo[col, k, 2] - own_geo[x, 2]
                strength = geo[col, k, 3] * own_geo[x, 3]
                if off_x == 0:
                    strength = jnp.where((sub == 3) & (k == 3), 0.0, strength)
                r2 = jnp.maximum(dx * dx + dy * dy + dzz * dzz, 1.0)
                ir = lax.rsqrt(r2)
                ir2 = ir * ir
                ir3 = ir * ir2
                u = r2 * (r2 * ir) * strength
                e = jnp.exp(-u)
                l3 = 1.0 - e
                l5 = l3 - u * e
                s = jnp.maximum(1.0 - r2 * (1.0 / CUT2), 0.0)
                si = s * s * ir3
                w3 = si * l3
                w5 = si * l5 * (3.0 * ir2)
                ax, ay, az = w5 * dx, w5 * dy, w5 * dzz
                tens[k, base + i, 0] = ax * dx - w3
                tens[k, base + i, 1] = ax * dy
                tens[k, base + i, 2] = ax * dzz
                tens[k, base + i, 3] = ay * dy - w3
                tens[k, base + i, 4] = ay * dzz
                tens[k, base + i, 5] = az * dzz - w3
            return carry

        lax.fori_loop(0, 7, body, 0)

    def apply(pair_list, base, start):
        used = sorted({x for x, _ in pair_list})

        def body(k, sums):
            sums = list(sums)
            for i, (x, col) in enumerate(pair_list):
                t = [tens[k, base + i, j] for j in range(6)]
                for s in range(2):
                    vx, vy, vz = (dip[col, k, 3 * s + j] for j in range(3))
                    o = 6 * x + 3 * s
                    sums[o] = sums[o] + (t[0] * vx + t[1] * vy + t[2] * vz)
                    sums[o + 1] = sums[o + 1] + (t[1] * vx + t[3] * vy + t[4] * vz)
                    sums[o + 2] = sums[o + 2] + (t[2] * vx + t[4] * vy + t[5] * vz)
            return tuple(sums)

        return lax.fori_loop(0, 7, body, start)

    def gather_field(phase):
        await_near(phase, False)
        if phase == 0:
            spread_geometry(OWN_COLS)
            tensors(OWN_PAIRS, 0)
        spread_dipoles(phase, OWN_COLS)
        sums = apply(OWN_PAIRS, 0, tuple(jnp.zeros((8, 128), F32) for _ in range(24)))
        for i in range(24):
            acc[i] = sums[i]
        await_near(phase, True)
        if phase == 0:
            spread_geometry(FAR_COLS)
            tensors(FAR_PAIRS, 16)
        spread_dipoles(phase, FAR_COLS)
        sums = apply(FAR_PAIRS, 16, tuple(acc[i] for i in range(24)))
        out = []
        for x in range(4):
            for c in range(6):
                rows[x, c : c + 1, :] = jnp.sum(sums[6 * x + c], axis=0, keepdims=True)
            out.append(jnp.where(sub < 6, rows[x], 0.0))
        return out

    def publish(phase, tiles):
        for x in range(4):
            vec[phase - 1, x] = tiles[x]
        vec_edge[phase - 1] = edge_of(tiles)
        send(phase)

    send(0)
    for x in range(4):
        for c in range(3):
            own_geo[x, c] = row_of(first, x, slice(c, c + 1))
        own_geo[x, 3] = THOLE * row_of(first, x, slice(3, 4))

    d0 = [src[x] * pol[x] for x in range(4)]
    field0 = gather_field(0)
    r0 = [src[x] - (d0[x] * ipol[x] - field0[x]) for x in range(4)]
    p0 = [pol[x] * r0[x] for x in range(4)]
    publish(1, p0)
    field1 = gather_field(1)
    y0 = [p0[x] * ipol[x] - field1[x] for x in range(4)]
    q0 = [pol[x] * y0[x] for x in range(4)]
    publish(2, q0)
    field2 = gather_field(2)
    z0 = [q0[x] * ipol[x] - field2[x] for x in range(4)]

    def dot(a, b):
        t = a[0] * b[0]
        for x in range(1, 4):
            t = t + a[x] * b[x]
        return jnp.sum(t, axis=1, keepdims=True)

    set_of = jnp.where(sub < 3, 0, 1)
    four = [dot(r0, p0), dot(p0, y0), dot(y0, q0), dot(q0, z0)]
    mix = jnp.zeros((8, 128), F32)
    for k in range(4):
        mix = jnp.where((lane >> 4) == 2 * k + set_of, four[k], mix)
    part[...] = jnp.sum(mix, axis=0, keepdims=True)

    def plane_copy(i, j, incoming):
        if incoming:
            i, j = -i % 4, -j % 4
        there, back = 4 * i + j, 4 * (-i % 4) + (-j % 4)
        return pltpu.make_async_remote_copy(
            src_ref=part, dst_ref=in_plane.at[back], send_sem=plane_send.at[there], recv_sem=plane_recv.at[back],
            device_id=at(i, j, 0), device_id_type=MESH,
        )

    def line_copy(k, incoming):
        if incoming:
            k = -k % 8
        return pltpu.make_async_remote_copy(
            src_ref=part2, dst_ref=in_line.at[-k % 8], send_sem=line_send.at[k], recv_sem=line_recv.at[-k % 8],
            device_id=at(0, 0, k), device_id_type=MESH,
        )

    others = [ij for ij in PLANE if ij != (0, 0)]
    for i, j in others:
        plane_copy(i, j, False).start()
    total = part[...]
    for i, j in others:
        plane_copy(i, j, True).wait_recv()
        total = total + in_plane[4 * i + j]
    part2[...] = total
    for k in range(1, 8):
        line_copy(k, False).start()
    for k in range(1, 8):
        line_copy(k, True).wait_recv()
        total = total + in_line[k]

    wide = jnp.broadcast_to(total, (8, 128))
    rz0, py, yq, qz = (
        jnp.sum(jnp.where(lane == 16 * (2 * k + set_of), wide, 0.0), axis=1, keepdims=True) for k in range(4)
    )
    gamma0 = rz0 / py
    rz1 = rz0 + gamma0 * (gamma0 * yq - 2.0 * py)
    keep = 1.0 + rz1 / rz0
    gamma1 = rz1 / (keep * (keep * py - 2.0 * gamma0 * yq) + gamma0 * gamma0 * qz)
    by_p = jnp.broadcast_to(gamma0 + gamma1 * keep, (8, 128))
    by_q = jnp.broadcast_to(gamma1 * gamma0, (8, 128))
    slot = lane
    for out, parts in ((dip_out, (d0, 1.0, p0, q0)), (res_out, (r0, -1.0, y0, z0))):
        base, sign, along, across = parts
        tile = [base[x] + sign * (by_p * along[x] - by_q * across[x]) for x in range(4)]
        for b in range(3):
            pick = 32 * ((slot >> 2) & 3) + 3 + 8 * b + (slot >> 4)
            got = [jnp.take_along_axis(tile[x], pick, axis=1) for x in range(4)]
            sx = slot & 3
            whole = jnp.where(sx == 0, got[0], jnp.where(sx == 1, got[1], jnp.where(sx == 2, got[2], got[3])))
            out[0, 0, b] = whole[0:6, :]

    for phase in range(3):
        for n in NEAR:
            copy(phase, n, False).wait_send()
    for i, j in others:
        plane_copy(i, j, False).wait_send()
    for k in range(1, 8):
        line_copy(k, False).wait_send()


def on_device(coords, polar, field, atom_count, pair_list):
    vmem = pl.BlockSpec(memory_space=pltpu.VMEM)
    smem = pl.BlockSpec(memory_space=pltpu.SMEM)
    tile = lambda *n: pltpu.VMEM(tuple(n) + (8, 128), F32)
    dma = lambda *n: pltpu.SemaphoreType.DMA(tuple(n))
    out = jax.ShapeDtypeStruct(field.shape, F32)
    return pl.pallas_call(
        kernel,
        out_shape=(out, out),
        in_specs=[vmem, vmem, vmem, smem, smem],
        out_specs=(vmem, vmem),
        scratch_shapes=[
            tile(3, 2),
            pltpu.VMEM((4, 16, 128), F32),
            pltpu.VMEM((16, 128), F32),
            tile(2, 4),
            tile(2),
            tile(4),
            tile(4),
            tile(4),
            tile(4, 4),
            pltpu.VMEM((8, 4, 16, 128), F32),
            pltpu.VMEM((18, 16, 128), F32),
            tile(2, 8, 4),
            tile(2, 18),
            tile(1),
            tile(10, 7),
            tile(10, 7, 4),
            tile(3, 7),
            tile(10, 7, 6),
            tile(7, 28, 6),
            tile(24),
            tile(4),
            pltpu.VMEM((1, 128), F32),
            pltpu.VMEM((16, 1, 128), F32),
            pltpu.VMEM((1, 128), F32),
            pltpu.VMEM((8, 1, 128), F32),
            dma(3, 26), dma(3, 26), dma(16), dma(16), dma(8), dma(8),
        ],
        compiler_params=pltpu.CompilerParams(collective_id=0, has_side_effects=True),
    )(coords, polar, field, atom_count, pair_list)


def solution(mesh):
    spec = P("gx", "gy", "gz")
    return jax.shard_map(
        on_device, mesh=mesh, in_specs=(spec,) * 5, out_specs=(spec, spec), check_vma=False,
    )
```

```python
import functools

import jax
import jax.numpy as jnp
from jax import lax
from jax.experimental import pallas as pl
from jax.experimental.pallas import tpu as pltpu
from jax.sharding import PartitionSpec as P


F32 = jnp.float32
I32 = jnp.int32
MESH = pl.DeviceIdType.MESH
SPACING = 2.2
HIGH = 2.1875
LOW = 0.0125
CUT2 = 49.0
THOLE = 0.39
SIZES = {"gx": 4, "gy": 4, "gz": 8}

NEAR = [(ox, oy, oz) for ox in (-1, 0, 1) for oy in (-1, 0, 1) for oz in (-1, 0, 1) if (ox, oy, oz) != (0, 0, 0)]
NEAR_ID = {n: i for i, n in enumerate(NEAR)}
FLAT = [n for n in NEAR if n[2] == 0]
FLAT_ID = {n: i for i, n in enumerate(FLAT)}
EDGE = [n for n in NEAR if n[2] != 0]
EDGE_ID = {n: i for i, n in enumerate(EDGE)}
PLANE = [(i, j) for i in range(4) for j in range(4)]
OWN_COLS = [3, 4, 5, 6]
FAR_COLS = [0, 1, 2, 7, 8, 9]
OWN_PAIRS = [(x, c) for c in OWN_COLS for x in range(4)]
FAR_PAIRS = [(x, c) for c in FAR_COLS for x in range(4) if abs(c - 3 - x) <= 3]


def col_home(col):
    return (-1, col + 1) if col < 3 else (0, col - 3) if col < 7 else (1, col - 7)


def lanes():
    return lax.broadcasted_iota(I32, (8, 128), 1)


def subs():
    return lax.broadcasted_iota(I32, (8, 128), 0)


def row_of(ref, *where):
    return jnp.broadcast_to(ref[where], (8, 128))


def kernel(
    coords_hbm, polar_hbm, field_hbm, count_hbm, pairs_hbm, dip_out, res_out,
    coords, polar, field, count, pairs, arg_sem,
    packed, first, first_edge, vec, vec_edge, src, pol, ipol, own_geo,
    in_first, in_first_edge, in_vec, in_vec_edge, ext, merged, geo, act, dip, tens, acc, rows,
    part, in_plane, part2, in_line,
    send_sem, recv_sem, plane_send, plane_recv, line_send, line_recv,
):
    me = {a: lax.axis_index(a) for a in SIZES}

    def at(ox, oy, oz):
        off = {"gx": ox, "gy": oy, "gz": oz}
        return {a: lax.rem(me[a] + off[a] % SIZES[a], SIZES[a]) for a in SIZES}

    barrier = pltpu.get_barrier_semaphore()
    for ox, oy, oz in NEAR:
        pl.semaphore_signal(barrier, inc=1, device_id=at(ox, oy, oz), device_id_type=MESH)

    loads = [
        pltpu.make_async_copy(a, b, arg_sem.at[i])
        for i, (a, b) in enumerate(
            ((coords_hbm, coords), (polar_hbm, polar), (field_hbm, field), (count_hbm, count), (pairs_hbm, pairs))
        )
    ]
    for load in loads:
        load.start()
    lane, sub = lanes(), subs()
    l32 = lane & 31
    zz = l32 - 3
    group = lane >> 5
    blk = zz >> 3
    valid = (zz >= 0) & (zz < 24)
    dz = 3 - sub

    for load in loads:
        load.wait()
    for b in range(3):
        slot = lane
        mask = (slot[0:1] < count[0, b]).astype(F32)
        packed[b, 0] = jnp.zeros((8, 128), F32)
        packed[b, 1] = jnp.zeros((8, 128), F32)
        for c in range(6):
            packed[b, 0, c : c + 1, :] = field[6 * b + c] * mask
        pol_row = polar[b]
        packed[b, 0, 6:7, :] = pol_row
        s1 = slot[0:1]
        for c, step in enumerate((s1 & 3, (s1 >> 2) & 3, s1 >> 4)):
            site = step.astype(F32) + 0.5
            packed[b, 1, c : c + 1, :] = (coords[3 * b + c] - site * HIGH) - site * LOW
        packed[b, 1, 3:4, :] = mask * lax.rsqrt(pol_row)
    bits = []
    for b in range(3):
        word = jnp.int32(0)
        for k in range(13):
            word = word | (jnp.int32(1) << (pairs[b, 0, k] & 31))
        bits.append(word)
    word = jnp.where(blk <= 0, bits[0], jnp.where(blk == 1, bits[1], bits[2]))
    for x in range(4):
        pick = 16 * (zz & 7) + 4 * group + x
        tile = []
        for t in range(2):
            got = [jnp.take_along_axis(packed[b, t], pick, axis=1) for b in range(3)]
            tile.append(jnp.where(valid, jnp.where(blk == 0, got[0], jnp.where(blk == 1, got[1], got[2])), 0.0))
        code = jnp.where(sub == 7, 14, jnp.maximum(15 + 3 * x + sub - 4, 0))
        flag = (lax.shift_right_logical(word, code) & 1).astype(F32)
        first[x, 0:8, :] = jnp.where((sub >= 4) & valid, flag, tile[1])
        src[x] = jnp.where(sub < 6, tile[0], 0.0)
        rows[x] = jnp.where((sub == 6) & valid, tile[0], 1.0)
        p = row_of(rows, x, slice(6, 7))
        pol[x] = p
        ipol[x] = 1.0 / p
        first[x, 8:16, :] = src[x] * p

    def edge_of(tiles):
        out = jnp.zeros((8, 128), F32)
        for x in range(4):
            top = pltpu.roll(tiles[x], (8 * x - 24) % 128, 1)
            low = pltpu.roll(tiles[x], (8 * x + 1) % 128, 1)
            out = jnp.where((l32 >= 8 * x) & (l32 < 8 * x + 3), top, out)
            out = jnp.where((l32 >= 8 * x + 4) & (l32 < 8 * x + 7), low, out)
        return out

    first_edge[0:8, :] = edge_of([first[x, 0:8, :] for x in range(4)])
    first_edge[8:16, :] = edge_of([first[x, 8:16, :] for x in range(4)])

    pl.semaphore_wait(barrier, len(NEAR))

    def copy(phase, n, incoming):
        ox, oy, oz = n if not incoming else tuple(-v for v in n)
        back = (-ox, -oy, -oz)
        count_rows = 14 if phase == 0 else 6
        if oz == 0:
            lo, hi = (1, 4) if ox == 1 else (0, 3) if ox == -1 else (0, 4)
            if phase == 0:
                s, d = first, in_first.at[FLAT_ID[back]]
            else:
                s, d = vec.at[phase - 1], in_vec.at[phase - 1, FLAT_ID[back]]
            s, d = s.at[lo:hi, 0:count_rows, :], d.at[lo:hi, 0:count_rows, :]
        else:
            if phase == 0:
                s, d = first_edge, in_first_edge.at[EDGE_ID[back]]
            else:
                s, d = vec_edge.at[phase - 1], in_vec_edge.at[phase - 1, EDGE_ID[back]]
            s, d = s.at[0:count_rows, :], d.at[0:count_rows, :]
        return pltpu.make_async_remote_copy(
            src_ref=s, dst_ref=d,
            send_sem=send_sem.at[phase, NEAR_ID[(ox, oy, oz)]], recv_sem=recv_sem.at[phase, NEAR_ID[back]],
            device_id=at(ox, oy, oz), device_id_type=MESH,
        )

    ORDER = sorted(NEAR, key=lambda n: (n[0] == 0, -sum(map(abs, n))))

    def send(phase):
        for n in sorted(NEAR, key=lambda n: (n[2] != 0, -sum(map(abs, n)))):
            copy(phase, n, False).start()

    def await_near(phase, far):
        for n in ORDER:
            if (n[0] != 0) == far:
                copy(phase, n, True).wait_recv()

    def ext_tile(phase, r0, ox, oy, x):
        if phase == 0:
            here = first[x, r0 : r0 + 8, :] if (ox, oy) == (0, 0) else in_first[FLAT_ID[(ox, oy, 0)], x, r0 : r0 + 8, :]
            low = in_first_edge[EDGE_ID[(ox, oy, -1)], r0 : r0 + 8, :]
            top = in_first_edge[EDGE_ID[(ox, oy, 1)], r0 : r0 + 8, :]
        else:
            here = vec[phase - 1, x] if (ox, oy) == (0, 0) else in_vec[phase - 1, FLAT_ID[(ox, oy, 0)], x]
            low = in_vec_edge[phase - 1, EDGE_ID[(ox, oy, -1)]]
            top = in_vec_edge[phase - 1, EDGE_ID[(ox, oy, 1)]]
        low = pltpu.roll(low, (-8 * x) % 128, 1)
        top = pltpu.roll(top, (23 - 8 * x) % 128, 1)
        return jnp.where(l32 < 3, low, jnp.where(l32 >= 27, top, here))

    def slide(ref, where, shift):
        return pltpu.roll(row_of(ref, *where), shift % 128, 1, stride=1, stride_axis=0)

    def merge_column(phase, r0, col):
        ox, x = col_home(col)
        tiles = {oy: ext_tile(phase, r0, ox, oy, x) for oy in (-1, 0, 1)}
        for k in range(7):
            dy = k - 3
            if dy > 0:
                tile = jnp.where(group < dy, tiles[1], tiles[0])
            elif dy < 0:
                tile = jnp.where(group >= 4 + dy, tiles[-1], tiles[0])
            else:
                tile = pltpu.roll(tiles[0], 64, 1)
            merged[col, k] = tile
        return tiles

    def merged_shift(k):
        return -32 * (k - 3) - 3 - (64 if k == 3 else 0)

    def spread_dipoles(phase, cols):
        for col in cols:
            merge_column(phase, 8 if phase == 0 else 0, col)
        for col in cols:
            for k in range(7):
                for c in range(6):
                    dip[col, k, c] = slide(merged, (col, k, slice(c, c + 1)), merged_shift(k))

    zp = zz + dz
    oz = (lax.shift_right_arithmetic(zp + 8, 3)) - (lax.shift_right_arithmetic(zz + 8, 3))
    lawful = valid & (sub < 7)

    def forward_act(ox, oy):
        x = 0 if ox == 0 else 2 + oy
        k = [row_of(first, x, slice(4 + i, 5 + i)) for i in range(3)]
        return jnp.where(oz == 0, k[1], jnp.where(oz > 0, k[2], k[0]))

    def backward_act(ox, oy):
        x = 0 if ox == 0 else 2 - oy
        ext[0] = ext_tile(0, 0, ox, oy, x)
        k = [slide(ext, (0, slice(4 + i, 5 + i)), -35) for i in range(3)]
        return jnp.where(oz == 0, k[1], jnp.where(oz > 0, k[0], k[2]))

    def self_act():
        ext[0] = ext_tile(0, 0, 0, 0, 0)
        up = row_of(first, 0, slice(7, 8))
        down = slide(ext, (0, slice(7, 8)), -35)
        return jnp.where(oz == 0, 1.0, jnp.where(oz > 0, up, down))

    def acts(ox):
        if ox == 0:
            a = {-1: backward_act(0, -1), 0: self_act(), 1: forward_act(0, 1)}
        else:
            a = {oy: (forward_act if ox > 0 else backward_act)(ox, oy) for oy in (-1, 0, 1)}
        for k in range(7):
            to = group + (k - 3)
            tile = jnp.where(to < 0, a[-1], jnp.where(to > 3, a[1], a[0]))
            act[ox + 1, k] = jnp.where(lawful, tile, 0.0)

    def spread_geometry(cols):
        for ox in sorted({col_home(c)[0] for c in cols}):
            acts(ox)
        for col in cols:
            merge_column(0, 0, col)
        for col in cols:
            ox, x = col_home(col)
            for k in range(7):
                for c in range(4):
                    tile = slide(merged, (col, k, slice(c, c + 1)), merged_shift(k))
                    if c == 2:
                        tile = tile + SPACING * dz.astype(F32)
                    if c == 3:
                        tile = tile * act[ox + 1, k]
                    geo[col, k, c] = tile

    def tensors(pair_list, base):
        def body(k, carry):
            shift_y = SPACING * (k - 3).astype(F32)
            for i, (x, col) in enumerate(pair_list):
                off_x = col - 3 - x
                dx = geo[col, k, 0] - own_geo[x, 0]
                if off_x:
                    dx = dx + SPACING * off_x
                dy = geo[col, k, 1] - own_geo[x, 1] + shift_y
                dzz = geo[col, k, 2] - own_geo[x, 2]
                strength = geo[col, k, 3] * own_geo[x, 3]
                if off_x == 0:
                    strength = jnp.where((sub == 3) & (k == 3), 0.0, strength)
                r2 = jnp.maximum(dx * dx + dy * dy + dzz * dzz, 1.0)
                ir = lax.rsqrt(r2)
                ir2 = ir * ir
                ir3 = ir * ir2
                u = r2 * (r2 * ir) * strength
                e = jnp.exp(-u)
                l3 = 1.0 - e
                l5 = l3 - u * e
                s = jnp.maximum(1.0 - r2 * (1.0 / CUT2), 0.0)
                si = s * s * ir3
                w3 = si * l3
                w5 = si * l5 * (3.0 * ir2)
                ax, ay, az = w5 * dx, w5 * dy, w5 * dzz
                tens[k, base + i, 0] = ax * dx - w3
                tens[k, base + i, 1] = ax * dy
                tens[k, base + i, 2] = ax * dzz
                tens[k, base + i, 3] = ay * dy - w3
                tens[k, base + i, 4] = ay * dzz
                tens[k, base + i, 5] = az * dzz - w3
            return carry

        lax.fori_loop(0, 7, body, 0)

    def apply(pair_list, base, start):
        used = sorted({x for x, _ in pair_list})

        def body(k, sums):
            sums = list(sums)
            for i, (x, col) in enumerate(pair_list):
                t = [tens[k, base + i, j] for j in range(6)]
                for s in range(2):
                    vx, vy, vz = (dip[col, k, 3 * s + j] for j in range(3))
                    o = 6 * x + 3 * s
                    sums[o] = sums[o] + (t[0] * vx + t[1] * vy + t[2] * vz)
                    sums[o + 1] = sums[o + 1] + (t[1] * vx + t[3] * vy + t[4] * vz)
                    sums[o + 2] = sums[o + 2] + (t[2] * vx + t[4] * vy + t[5] * vz)
            return tuple(sums)

        return lax.fori_loop(0, 7, body, start)

    def gather_field(phase):
        await_near(phase, False)
        if phase == 0:
            spread_geometry(OWN_COLS)
            tensors(OWN_PAIRS, 0)
        spread_dipoles(phase, OWN_COLS)
        sums = apply(OWN_PAIRS, 0, tuple(jnp.zeros((8, 128), F32) for _ in range(24)))
        for i in range(24):
            acc[i] = sums[i]
        await_near(phase, True)
        if phase == 0:
            spread_geometry(FAR_COLS)
            tensors(FAR_PAIRS, 16)
        spread_dipoles(phase, FAR_COLS)
        sums = apply(FAR_PAIRS, 16, tuple(acc[i] for i in range(24)))
        out = []
        for x in range(4):
            for c in range(6):
                rows[x, c : c + 1, :] = jnp.sum(sums[6 * x + c], axis=0, keepdims=True)
            out.append(jnp.where(sub < 6, rows[x], 0.0))
        return out

    def publish(phase, tiles):
        for x in range(4):
            vec[phase - 1, x] = tiles[x]
        vec_edge[phase - 1] = edge_of(tiles)
        send(phase)

    send(0)
    for x in range(4):
        for c in range(3):
            own_geo[x, c] = row_of(first, x, slice(c, c + 1))
        own_geo[x, 3] = THOLE * row_of(first, x, slice(3, 4))

    d0 = [src[x] * pol[x] for x in range(4)]
    field0 = gather_field(0)
    r0 = [src[x] - (d0[x] * ipol[x] - field0[x]) for x in range(4)]
    p0 = [pol[x] * r0[x] for x in range(4)]
    publish(1, p0)
    field1 = gather_field(1)
    y0 = [p0[x] * ipol[x] - field1[x] for x in range(4)]
    q0 = [pol[x] * y0[x] for x in range(4)]
    publish(2, q0)
    field2 = gather_field(2)
    z0 = [q0[x] * ipol[x] - field2[x] for x in range(4)]

    def dot(a, b):
        t = a[0] * b[0]
        for x in range(1, 4):
            t = t + a[x] * b[x]
        return jnp.sum(t, axis=1, keepdims=True)

    set_of = jnp.where(sub < 3, 0, 1)
    four = [dot(r0, p0), dot(p0, y0), dot(y0, q0), dot(q0, z0)]
    mix = jnp.zeros((8, 128), F32)
    for k in range(4):
        mix = jnp.where((lane >> 4) == 2 * k + set_of, four[k], mix)
    part[...] = jnp.sum(mix, axis=0, keepdims=True)

    def plane_copy(i, j, incoming):
        if incoming:
            i, j = -i % 4, -j % 4
        there, back = 4 * i + j, 4 * (-i % 4) + (-j % 4)
        return pltpu.make_async_remote_copy(
            src_ref=part, dst_ref=in_plane.at[back], send_sem=plane_send.at[there], recv_sem=plane_recv.at[back],
            device_id=at(i, j, 0), device_id_type=MESH,
        )

    def line_copy(k, incoming):
        if incoming:
            k = -k % 8
        return pltpu.make_async_remote_copy(
            src_ref=part2, dst_ref=in_line.at[-k % 8], send_sem=line_send.at[k], recv_sem=line_recv.at[-k % 8],
            device_id=at(0, 0, k), device_id_type=MESH,
        )

    others = [ij for ij in PLANE if ij != (0, 0)]
    for i, j in others:
        plane_copy(i, j, False).start()
    total = part[...]
    for i, j in others:
        plane_copy(i, j, True).wait_recv()
        total = total + in_plane[4 * i + j]
    part2[...] = total
    for k in range(1, 8):
        line_copy(k, False).start()
    for k in range(1, 8):
        line_copy(k, True).wait_recv()
        total = total + in_line[k]

    wide = jnp.broadcast_to(total, (8, 128))
    rz0, py, yq, qz = (
        jnp.sum(jnp.where(lane == 16 * (2 * k + set_of), wide, 0.0), axis=1, keepdims=True) for k in range(4)
    )
    gamma0 = rz0 / py
    rz1 = rz0 + gamma0 * (gamma0 * yq - 2.0 * py)
    keep = 1.0 + rz1 / rz0
    gamma1 = rz1 / (keep * (keep * py - 2.0 * gamma0 * yq) + gamma0 * gamma0 * qz)
    by_p = jnp.broadcast_to(gamma0 + gamma1 * keep, (8, 128))
    by_q = jnp.broadcast_to(gamma1 * gamma0, (8, 128))
    slot = lane
    for out, parts in ((dip_out, (d0, 1.0, p0, q0)), (res_out, (r0, -1.0, y0, z0))):
        base, sign, along, across = parts
        tile = [base[x] + sign * (by_p * along[x] - by_q * across[x]) for x in range(4)]
        for b in range(3):
            pick = 32 * ((slot >> 2) & 3) + 3 + 8 * b + (slot >> 4)
            got = [jnp.take_along_axis(tile[x], pick, axis=1) for x in range(4)]
            sx = slot & 3
            whole = jnp.where(sx == 0, got[0], jnp.where(sx == 1, got[1], jnp.where(sx == 2, got[2], got[3])))
            for c in range(6):
                out[6 * b + c] = whole[c : c + 1, :]

    for phase in range(3):
        for n in NEAR:
            copy(phase, n, False).wait_send()
    for i, j in others:
        plane_copy(i, j, False).wait_send()
    for k in range(1, 8):
        line_copy(k, False).wait_send()


def on_device(coords, polar, field, atom_count, pair_list):
    vmem = pl.BlockSpec(memory_space=pltpu.VMEM)
    tile = lambda *n: pltpu.VMEM(tuple(n) + (8, 128), F32)
    dma = lambda *n: pltpu.SemaphoreType.DMA(tuple(n))
    out = jax.ShapeDtypeStruct((18, 1, 128), F32)
    dipoles, residual = pl.pallas_call(
        kernel,
        out_shape=(out, out),
        in_specs=[pl.BlockSpec(memory_space=pl.ANY)] * 5,
        out_specs=(vmem, vmem),
        scratch_shapes=[
            pltpu.VMEM((9, 1, 128), F32),
            pltpu.VMEM((3, 1, 128), F32),
            pltpu.VMEM((18, 1, 128), F32),
            pltpu.SMEM((1, 3), I32),
            pltpu.SMEM((3, 1, 13), I32),
            dma(5),
            tile(3, 2),
            pltpu.VMEM((4, 16, 128), F32),
            pltpu.VMEM((16, 128), F32),
            tile(2, 4),
            tile(2),
            tile(4),
            tile(4),
            tile(4),
            tile(4, 4),
            pltpu.VMEM((8, 4, 16, 128), F32),
            pltpu.VMEM((18, 16, 128), F32),
            tile(2, 8, 4),
            tile(2, 18),
            tile(1),
            tile(10, 7),
            tile(10, 7, 4),
            tile(3, 7),
            tile(10, 7, 6),
            tile(7, 28, 6),
            tile(24),
            tile(4),
            pltpu.VMEM((1, 128), F32),
            pltpu.VMEM((16, 1, 128), F32),
            pltpu.VMEM((1, 128), F32),
            pltpu.VMEM((8, 1, 128), F32),
            dma(3, 26), dma(3, 26), dma(16), dma(16), dma(8), dma(8),
        ],
        compiler_params=pltpu.CompilerParams(collective_id=0, has_side_effects=True),
    )(
        coords.reshape(9, 1, 128), polar.reshape(3, 1, 128), field.reshape(18, 1, 128),
        atom_count.reshape(1, 3), pair_list.reshape(3, 1, 13),
    )
    return dipoles.reshape(field.shape), residual.reshape(field.shape)


def solution(mesh):
    spec = P("gx", "gy", "gz")
    return jax.shard_map(
        on_device, mesh=mesh, in_specs=(spec,) * 5, out_specs=(spec, spec), check_vma=False,
    )
```

```python
import functools

import jax
import jax.numpy as jnp
from jax import lax
from jax.experimental import pallas as pl
from jax.experimental.pallas import tpu as pltpu
from jax.sharding import PartitionSpec as P


F32 = jnp.float32
I32 = jnp.int32
MESH = pl.DeviceIdType.MESH
SPACING = 2.2
HIGH = 2.1875
LOW = 0.0125
CUT2 = 49.0
THOLE = 0.39
SIZES = {"gx": 4, "gy": 4, "gz": 8}

NEAR = [(ox, oy, oz) for ox in (-1, 0, 1) for oy in (-1, 0, 1) for oz in (-1, 0, 1) if (ox, oy, oz) != (0, 0, 0)]
NEAR_ID = {n: i for i, n in enumerate(NEAR)}
FLAT = [n for n in NEAR if n[2] == 0]
FLAT_ID = {n: i for i, n in enumerate(FLAT)}
EDGE = [n for n in NEAR if n[2] != 0]
EDGE_ID = {n: i for i, n in enumerate(EDGE)}


def ring(k):
    return min(k, 4 - k)


def stage_group(xs, zs, ys, cores):
    every = [(x, z, y, c) for x in range(xs) for z in range(zs) for y in range(ys) for c in range(cores)]
    return sorted(every[1:], key=lambda n: -sum(map(ring, n[:3])))


STAGES = [stage_group(1, 1, 1, 2), stage_group(4, 4, 4, 1)]

OWN_COLS = [3, 4, 5, 6]
FAR_COLS = [0, 1, 2, 7, 8, 9]
OWN_PAIRS = [(x, c) for c in OWN_COLS for x in range(4)]
FAR_PAIRS = [(x, c) for c in FAR_COLS for x in range(4) if abs(c - 3 - x) <= 3]


def col_home(col):
    return (-1, col + 1) if col < 3 else (0, col - 3) if col < 7 else (1, col - 7)


def lanes():
    return lax.broadcasted_iota(I32, (8, 128), 1)


def subs():
    return lax.broadcasted_iota(I32, (8, 128), 0)


def row_of(ref, *where):
    return jnp.broadcast_to(ref[where], (8, 128))


def kernel(
    coords_hbm, polar_hbm, field_hbm, count_hbm, pairs_hbm, dip_out, res_out,
    coords, polar, field, count, pairs, arg_sem,
    packed, first, first_edge, vec, vec_edge, src, pol, ipol, own_geo,
    in_first, in_first_edge, in_vec, in_vec_edge, ext, merged, geo, act, dip, tens, acc, rows,
    part, send_sem, recv_sem, *sums,
):
    in_sum, sum_send, sum_recv = (sums[i :: 3] for i in range(3))
    me = {a: lax.axis_index(a) for a in SIZES}

    def at(ox, oy, oz):
        off = {"gx": ox, "gy": oy, "gz": oz}
        return {a: lax.rem(me[a] + off[a] % SIZES[a], SIZES[a]) for a in SIZES}

    barrier = pltpu.get_barrier_semaphore()
    for ox, oy, oz in NEAR:
        pl.semaphore_signal(barrier, inc=1, device_id=at(ox, oy, oz), device_id_type=MESH)

    loads = [
        pltpu.make_async_copy(a, b, arg_sem.at[i])
        for i, (a, b) in enumerate(
            ((coords_hbm, coords), (polar_hbm, polar), (field_hbm, field), (count_hbm, count), (pairs_hbm, pairs))
        )
    ]
    for load in loads:
        load.start()
    lane, sub = lanes(), subs()
    l32 = lane & 31
    zz = l32 - 3
    group = lane >> 5
    blk = zz >> 3
    valid = (zz >= 0) & (zz < 24)
    dz = 3 - sub

    for load in loads:
        load.wait()
    for b in range(3):
        slot = lane
        mask = (slot[0:1] < count[0, b]).astype(F32)
        packed[b, 0] = jnp.zeros((8, 128), F32)
        packed[b, 1] = jnp.zeros((8, 128), F32)
        for c in range(6):
            packed[b, 0, c : c + 1, :] = field[6 * b + c] * mask
        pol_row = polar[b]
        packed[b, 0, 6:7, :] = pol_row
        s1 = slot[0:1]
        for c, step in enumerate((s1 & 3, (s1 >> 2) & 3, s1 >> 4)):
            site = step.astype(F32) + 0.5
            packed[b, 1, c : c + 1, :] = (coords[3 * b + c] - site * HIGH) - site * LOW
        packed[b, 1, 3:4, :] = mask * lax.rsqrt(pol_row)
    bits = []
    for b in range(3):
        word = jnp.int32(0)
        for k in range(13):
            word = word | (jnp.int32(1) << (pairs[b, 0, k] & 31))
        bits.append(word)
    word = jnp.where(blk <= 0, bits[0], jnp.where(blk == 1, bits[1], bits[2]))
    for x in range(4):
        pick = 16 * (zz & 7) + 4 * group + x
        tile = []
        for t in range(2):
            got = [jnp.take_along_axis(packed[b, t], pick, axis=1) for b in range(3)]
            tile.append(jnp.where(valid, jnp.where(blk == 0, got[0], jnp.where(blk == 1, got[1], got[2])), 0.0))
        code = jnp.where(sub == 7, 14, jnp.maximum(15 + 3 * x + sub - 4, 0))
        flag = (lax.shift_right_logical(word, code) & 1).astype(F32)
        first[x, 0:8, :] = jnp.where((sub >= 4) & valid, flag, tile[1])
        src[x] = jnp.where(sub < 6, tile[0], 0.0)
        rows[x] = jnp.where((sub == 6) & valid, tile[0], 1.0)
        p = row_of(rows, x, slice(6, 7))
        pol[x] = p
        ipol[x] = 1.0 / p
        first[x, 8:16, :] = src[x] * p

    def edge_of(tiles):
        out = jnp.zeros((8, 128), F32)
        for x in range(4):
            top = pltpu.roll(tiles[x], (8 * x - 24) % 128, 1)
            low = pltpu.roll(tiles[x], (8 * x + 1) % 128, 1)
            out = jnp.where((l32 >= 8 * x) & (l32 < 8 * x + 3), top, out)
            out = jnp.where((l32 >= 8 * x + 4) & (l32 < 8 * x + 7), low, out)
        return out

    first_edge[0:8, :] = edge_of([first[x, 0:8, :] for x in range(4)])
    first_edge[8:16, :] = edge_of([first[x, 8:16, :] for x in range(4)])

    pl.semaphore_wait(barrier, len(NEAR))

    def copy(phase, n, incoming):
        ox, oy, oz = n if not incoming else tuple(-v for v in n)
        back = (-ox, -oy, -oz)
        count_rows = 14 if phase == 0 else 6
        if oz == 0:
            lo, hi = (1, 4) if ox == 1 else (0, 3) if ox == -1 else (0, 4)
            if phase == 0:
                s, d = first, in_first.at[FLAT_ID[back]]
            else:
                s, d = vec.at[phase - 1], in_vec.at[phase - 1, FLAT_ID[back]]
            s, d = s.at[lo:hi, 0:count_rows, :], d.at[lo:hi, 0:count_rows, :]
        else:
            if phase == 0:
                s, d = first_edge, in_first_edge.at[EDGE_ID[back]]
            else:
                s, d = vec_edge.at[phase - 1], in_vec_edge.at[phase - 1, EDGE_ID[back]]
            s, d = s.at[0:count_rows, :], d.at[0:count_rows, :]
        return pltpu.make_async_remote_copy(
            src_ref=s, dst_ref=d,
            send_sem=send_sem.at[phase, NEAR_ID[(ox, oy, oz)]], recv_sem=recv_sem.at[phase, NEAR_ID[back]],
            device_id=at(ox, oy, oz), device_id_type=MESH,
        )

    ORDER = sorted(NEAR, key=lambda n: (n[0] == 0, -sum(map(abs, n))))

    def send(phase):
        for n in sorted(NEAR, key=lambda n: -sum(map(abs, n))):
            copy(phase, n, False).start()

    def await_near(phase, far):
        for n in ORDER:
            if (n[0] != 0) == far:
                copy(phase, n, True).wait_recv()

    def ext_tile(phase, r0, ox, oy, x):
        if phase == 0:
            here = first[x, r0 : r0 + 8, :] if (ox, oy) == (0, 0) else in_first[FLAT_ID[(ox, oy, 0)], x, r0 : r0 + 8, :]
            low = in_first_edge[EDGE_ID[(ox, oy, -1)], r0 : r0 + 8, :]
            top = in_first_edge[EDGE_ID[(ox, oy, 1)], r0 : r0 + 8, :]
        else:
            here = vec[phase - 1, x] if (ox, oy) == (0, 0) else in_vec[phase - 1, FLAT_ID[(ox, oy, 0)], x]
            low = in_vec_edge[phase - 1, EDGE_ID[(ox, oy, -1)]]
            top = in_vec_edge[phase - 1, EDGE_ID[(ox, oy, 1)]]
        low = pltpu.roll(low, (-8 * x) % 128, 1)
        top = pltpu.roll(top, (23 - 8 * x) % 128, 1)
        return jnp.where(l32 < 3, low, jnp.where(l32 >= 27, top, here))

    def slide(ref, where, shift):
        return pltpu.roll(row_of(ref, *where), shift % 128, 1, stride=1, stride_axis=0)

    def merge_column(phase, r0, col):
        ox, x = col_home(col)
        tiles = {oy: ext_tile(phase, r0, ox, oy, x) for oy in (-1, 0, 1)}
        for k in range(7):
            dy = k - 3
            if dy > 0:
                tile = jnp.where(group < dy, tiles[1], tiles[0])
            elif dy < 0:
                tile = jnp.where(group >= 4 + dy, tiles[-1], tiles[0])
            else:
                tile = pltpu.roll(tiles[0], 64, 1)
            merged[col, k] = tile
        return tiles

    def merged_shift(k):
        return -32 * (k - 3) - 3 - (64 if k == 3 else 0)

    def spread_dipoles(phase, cols):
        for col in cols:
            merge_column(phase, 8 if phase == 0 else 0, col)
        for col in cols:
            for k in range(7):
                for c in range(6):
                    dip[col, k, c] = slide(merged, (col, k, slice(c, c + 1)), merged_shift(k))

    zp = zz + dz
    oz = (lax.shift_right_arithmetic(zp + 8, 3)) - (lax.shift_right_arithmetic(zz + 8, 3))
    lawful = valid & (sub < 7)

    def forward_act(ox, oy):
        x = 0 if ox == 0 else 2 + oy
        k = [row_of(first, x, slice(4 + i, 5 + i)) for i in range(3)]
        return jnp.where(oz == 0, k[1], jnp.where(oz > 0, k[2], k[0]))

    def backward_act(ox, oy):
        x = 0 if ox == 0 else 2 - oy
        ext[0] = ext_tile(0, 0, ox, oy, x)
        k = [slide(ext, (0, slice(4 + i, 5 + i)), -35) for i in range(3)]
        return jnp.where(oz == 0, k[1], jnp.where(oz > 0, k[0], k[2]))

    def self_act():
        ext[0] = ext_tile(0, 0, 0, 0, 0)
        up = row_of(first, 0, slice(7, 8))
        down = slide(ext, (0, slice(7, 8)), -35)
        return jnp.where(oz == 0, 1.0, jnp.where(oz > 0, up, down))

    def acts(ox):
        if ox == 0:
            a = {-1: backward_act(0, -1), 0: self_act(), 1: forward_act(0, 1)}
        else:
            a = {oy: (forward_act if ox > 0 else backward_act)(ox, oy) for oy in (-1, 0, 1)}
        for k in range(7):
            to = group + (k - 3)
            tile = jnp.where(to < 0, a[-1], jnp.where(to > 3, a[1], a[0]))
            act[ox + 1, k] = jnp.where(lawful, tile, 0.0)

    def spread_geometry(cols):
        for ox in sorted({col_home(c)[0] for c in cols}):
            acts(ox)
        for col in cols:
            merge_column(0, 0, col)
        for col in cols:
            ox, x = col_home(col)
            for k in range(7):
                for c in range(4):
                    tile = slide(merged, (col, k, slice(c, c + 1)), merged_shift(k))
                    if c == 2:
                        tile = tile + SPACING * dz.astype(F32)
                    if c == 3:
                        tile = tile * act[ox + 1, k]
                    geo[col, k, c] = tile

    def tensors(pair_list, base):
        def body(k, carry):
            shift_y = SPACING * (k - 3).astype(F32)
            for i, (x, col) in enumerate(pair_list):
                off_x = col - 3 - x
                dx = geo[col, k, 0] - own_geo[x, 0]
                if off_x:
                    dx = dx + SPACING * off_x
                dy = geo[col, k, 1] - own_geo[x, 1] + shift_y
                dzz = geo[col, k, 2] - own_geo[x, 2]
                strength = geo[col, k, 3] * own_geo[x, 3]
                if off_x == 0:
                    strength = jnp.where((sub == 3) & (k == 3), 0.0, strength)
                r2 = jnp.maximum(dx * dx + dy * dy + dzz * dzz, 1.0)
                ir = lax.rsqrt(r2)
                ir2 = ir * ir
                ir3 = ir * ir2
                u = r2 * (r2 * ir) * strength
                e = jnp.exp(-u)
                l3 = 1.0 - e
                l5 = l3 - u * e
                s = jnp.maximum(1.0 - r2 * (1.0 / CUT2), 0.0)
                si = s * s * ir3
                w3 = si * l3
                w5 = si * l5 * (3.0 * ir2)
                ax, ay, az = w5 * dx, w5 * dy, w5 * dzz
                tens[k, base + i, 0] = ax * dx - w3
                tens[k, base + i, 1] = ax * dy
                tens[k, base + i, 2] = ax * dzz
                tens[k, base + i, 3] = ay * dy - w3
                tens[k, base + i, 4] = ay * dzz
                tens[k, base + i, 5] = az * dzz - w3
            return carry

        lax.fori_loop(0, 7, body, 0)

    def apply(pair_list, base, start):
        used = sorted({x for x, _ in pair_list})

        def body(k, sums):
            sums = list(sums)
            for i, (x, col) in enumerate(pair_list):
                t = [tens[k, base + i, j] for j in range(6)]
                for s in range(2):
                    vx, vy, vz = (dip[col, k, 3 * s + j] for j in range(3))
                    o = 6 * x + 3 * s
                    sums[o] = sums[o] + (t[0] * vx + t[1] * vy + t[2] * vz)
                    sums[o + 1] = sums[o + 1] + (t[1] * vx + t[3] * vy + t[4] * vz)
                    sums[o + 2] = sums[o + 2] + (t[2] * vx + t[4] * vy + t[5] * vz)
            return tuple(sums)

        return lax.fori_loop(0, 7, body, start)

    def gather_field(phase):
        await_near(phase, False)
        if phase == 0:
            spread_geometry(OWN_COLS)
            tensors(OWN_PAIRS, 0)
        spread_dipoles(phase, OWN_COLS)
        sums = apply(OWN_PAIRS, 0, tuple(jnp.zeros((8, 128), F32) for _ in range(24)))
        for i in range(24):
            acc[i] = sums[i]
        await_near(phase, True)
        if phase == 0:
            spread_geometry(FAR_COLS)
            tensors(FAR_PAIRS, 16)
        spread_dipoles(phase, FAR_COLS)
        sums = apply(FAR_PAIRS, 16, tuple(acc[i] for i in range(24)))
        out = []
        for x in range(4):
            for c in range(6):
                rows[x, c : c + 1, :] = jnp.sum(sums[6 * x + c], axis=0, keepdims=True)
            out.append(jnp.where(sub < 6, rows[x], 0.0))
        return out

    def publish(phase, tiles):
        for x in range(4):
            vec[phase - 1, x] = tiles[x]
        vec_edge[phase - 1] = edge_of(tiles)
        send(phase)

    send(0)
    for x in range(4):
        for c in range(3):
            own_geo[x, c] = row_of(first, x, slice(c, c + 1))
        own_geo[x, 3] = THOLE * row_of(first, x, slice(3, 4))

    d0 = [src[x] * pol[x] for x in range(4)]
    field0 = gather_field(0)
    r0 = [src[x] - (d0[x] * ipol[x] - field0[x]) for x in range(4)]
    p0 = [pol[x] * r0[x] for x in range(4)]
    publish(1, p0)
    field1 = gather_field(1)
    y0 = [p0[x] * ipol[x] - field1[x] for x in range(4)]
    q0 = [pol[x] * y0[x] for x in range(4)]
    publish(2, q0)
    field2 = gather_field(2)
    z0 = [q0[x] * ipol[x] - field2[x] for x in range(4)]

    def dot(a, b):
        t = a[0] * b[0]
        for x in range(1, 4):
            t = t + a[x] * b[x]
        return jnp.sum(t, axis=1, keepdims=True)

    set_of = jnp.where(sub < 3, 0, 1)
    four = [dot(r0, p0), dot(p0, y0), dot(y0, q0), dot(q0, z0)]
    mix = jnp.zeros((8, 128), F32)
    for k in range(4):
        mix = jnp.where((lane >> 4) == 2 * k + set_of, four[k], mix)
    total = jnp.sum(mix, axis=0, keepdims=True)

    def peer(x, z, y, core):
        chip = lax.rem((me["gz"] >> 1) + y % 4, 4)
        return {"gx": lax.rem(me["gx"] + x % 4, 4), "gy": lax.rem(me["gy"] + z % 4, 4),
                "gz": 2 * chip + ((me["gz"] & 1) ^ core)}

    def sum_copy(stage, n, incoming):
        x, z, y, core = n
        if incoming:
            x, z, y = -x % 4, -z % 4, -y % 4
        group = STAGES[stage]
        there, back = group.index((x, z, y, core)), group.index((-x % 4, -z % 4, -y % 4, core))
        return pltpu.make_async_remote_copy(
            src_ref=part.at[stage], dst_ref=in_sum[stage].at[back],
            send_sem=sum_send[stage].at[there], recv_sem=sum_recv[stage].at[back],
            device_id=peer(x, z, y, core), device_id_type=MESH,
        )

    for stage, group in enumerate(STAGES):
        part[stage] = total
        for n in group:
            sum_copy(stage, n, False).start()
        for n in reversed(group):
            sum_copy(stage, n, True).wait_recv()
        lot = [total] + [in_sum[stage][i] for i in range(len(group))]
        while len(lot) > 1:
            lot = [lot[i] + lot[i + 1] if i + 1 < len(lot) else lot[i] for i in range(0, len(lot), 2)]
        total = lot[0]

    wide = jnp.broadcast_to(total, (8, 128))
    rz0, py, yq, qz = (
        jnp.sum(jnp.where(lane == 16 * (2 * k + set_of), wide, 0.0), axis=1, keepdims=True) for k in range(4)
    )
    gamma0 = rz0 / py
    rz1 = rz0 + gamma0 * (gamma0 * yq - 2.0 * py)
    keep = 1.0 + rz1 / rz0
    gamma1 = rz1 / (keep * (keep * py - 2.0 * gamma0 * yq) + gamma0 * gamma0 * qz)
    by_p = jnp.broadcast_to(gamma0 + gamma1 * keep, (8, 128))
    by_q = jnp.broadcast_to(gamma1 * gamma0, (8, 128))
    slot = lane
    for out, parts in ((dip_out, (d0, 1.0, p0, q0)), (res_out, (r0, -1.0, y0, z0))):
        base, sign, along, across = parts
        tile = [base[x] + sign * (by_p * along[x] - by_q * across[x]) for x in range(4)]
        for b in range(3):
            pick = 32 * ((slot >> 2) & 3) + 3 + 8 * b + (slot >> 4)
            got = [jnp.take_along_axis(tile[x], pick, axis=1) for x in range(4)]
            sx = slot & 3
            whole = jnp.where(sx == 0, got[0], jnp.where(sx == 1, got[1], jnp.where(sx == 2, got[2], got[3])))
            for c in range(6):
                out[6 * b + c] = whole[c : c + 1, :]

    for phase in range(3):
        for n in NEAR:
            copy(phase, n, False).wait_send()
    for stage, group in enumerate(STAGES):
        for n in group:
            sum_copy(stage, n, False).wait_send()


def put_out(dipoles, residual, dip_out, res_out, sem):
    copies = [
        pltpu.make_async_copy(a, b, sem.at[i]) for i, (a, b) in enumerate(((dipoles, dip_out), (residual, res_out)))
    ]
    for copy in copies:
        copy.start()
    for copy in copies:
        copy.wait()


def on_device(coords, polar, field, atom_count, pair_list):
    vmem = pl.BlockSpec(memory_space=pltpu.VMEM)
    tile = lambda *n: pltpu.VMEM(tuple(n) + (8, 128), F32)
    dma = lambda *n: pltpu.SemaphoreType.DMA(tuple(n))
    kept = pltpu.VMEM((18, 1, 128), F32)
    dipoles, residual = pl.pallas_call(
        kernel,
        out_shape=(kept, kept),
        in_specs=[pl.BlockSpec(memory_space=pl.ANY)] * 5,
        out_specs=(vmem, vmem),
        scratch_shapes=[
            pltpu.VMEM((9, 1, 128), F32),
            pltpu.VMEM((3, 1, 128), F32),
            pltpu.VMEM((18, 1, 128), F32),
            pltpu.SMEM((1, 3), I32),
            pltpu.SMEM((3, 1, 13), I32),
            dma(5),
            tile(3, 2),
            pltpu.VMEM((4, 16, 128), F32),
            pltpu.VMEM((16, 128), F32),
            tile(2, 4),
            tile(2),
            tile(4),
            tile(4),
            tile(4),
            tile(4, 4),
            pltpu.VMEM((8, 4, 16, 128), F32),
            pltpu.VMEM((18, 16, 128), F32),
            tile(2, 8, 4),
            tile(2, 18),
            tile(1),
            tile(10, 7),
            tile(10, 7, 4),
            tile(3, 7),
            tile(10, 7, 6),
            tile(7, 28, 6),
            tile(24),
            tile(4),
            pltpu.VMEM((len(STAGES), 1, 128), F32),
            dma(3, 26), dma(3, 26),
            *(s for g in STAGES for s in (pltpu.VMEM((len(g), 1, 128), F32), dma(len(g)), dma(len(g)))),
        ],
        compiler_params=pltpu.CompilerParams(collective_id=0, has_side_effects=True),
    )(
        coords.reshape(9, 1, 128), polar.reshape(3, 1, 128), field.reshape(18, 1, 128),
        atom_count.reshape(1, 3), pair_list.reshape(3, 1, 13),
    )
    out = jax.ShapeDtypeStruct((18, 1, 128), F32)
    anywhere = pl.BlockSpec(memory_space=pl.ANY)
    dipoles, residual = pl.pallas_call(
        put_out, out_shape=(out, out), in_specs=[vmem] * 2, out_specs=(anywhere,) * 2, scratch_shapes=[dma(2)],
    )(*(pltpu.with_memory_space_constraint(v, pltpu.VMEM) for v in (dipoles, residual)))
    return dipoles.reshape(field.shape), residual.reshape(field.shape)


def solution(mesh):
    spec = P("gx", "gy", "gz")
    return jax.shard_map(
        on_device, mesh=mesh, in_specs=(spec,) * 5, out_specs=(spec, spec), check_vma=False,
    )
```

```python
import functools

import jax
import jax.numpy as jnp
from jax import lax
from jax.experimental import pallas as pl
from jax.experimental.pallas import tpu as pltpu
from jax.sharding import PartitionSpec as P


F32 = jnp.float32
I32 = jnp.int32
MESH = pl.DeviceIdType.MESH
SPACING = 2.2
HIGH = 2.1875
LOW = 0.0125
CUT2 = 49.0
THOLE = 0.39
SIZES = {"gx": 4, "gy": 4, "gz": 8}

NEAR = [(ox, oy, oz) for ox in (-1, 0, 1) for oy in (-1, 0, 1) for oz in (-1, 0, 1) if (ox, oy, oz) != (0, 0, 0)]
NEAR_ID = {n: i for i, n in enumerate(NEAR)}
FLAT = [n for n in NEAR if n[2] == 0]
FLAT_ID = {n: i for i, n in enumerate(FLAT)}
EDGE = [n for n in NEAR if n[2] != 0]
EDGE_ID = {n: i for i, n in enumerate(EDGE)}


def ring(k):
    return min(k, 4 - k)


def stage_group(xs, zs, ys, cores):
    every = [(x, z, y, c) for x in range(xs) for z in range(zs) for y in range(ys) for c in range(cores)]
    return sorted(every[1:], key=lambda n: -sum(map(ring, n[:3])))


STAGES = [stage_group(1, 1, 1, 2), stage_group(4, 4, 4, 1)]

OWN_COLS = [3, 4, 5, 6]
FAR_COLS = [0, 1, 2, 7, 8, 9]
OWN_PAIRS = [(x, c) for c in OWN_COLS for x in range(4)]
FAR_PAIRS = [(x, c) for c in FAR_COLS for x in range(4) if abs(c - 3 - x) <= 3]


def col_home(col):
    return (-1, col + 1) if col < 3 else (0, col - 3) if col < 7 else (1, col - 7)


def lanes():
    return lax.broadcasted_iota(I32, (8, 128), 1)


def subs():
    return lax.broadcasted_iota(I32, (8, 128), 0)


def row_of(ref, *where):
    return jnp.broadcast_to(ref[where], (8, 128))


def kernel(
    coords_hbm, polar_hbm, field_hbm, count_hbm, pairs_hbm, dip_out, res_out,
    coords, polar, field, count, pairs, arg_sem,
    packed, first, first_edge, vec, vec_edge, src, pol, ipol, own_geo,
    in_first, in_first_edge, in_vec, in_vec_edge, ext, merged, geo, act, dip, tens, acc, rows,
    part, send_sem, recv_sem, *sums,
):
    in_sum, sum_send, sum_recv = (sums[i :: 3] for i in range(3))
    me = {a: lax.axis_index(a) for a in SIZES}

    def at(ox, oy, oz):
        off = {"gx": ox, "gy": oy, "gz": oz}
        return {a: lax.rem(me[a] + off[a] % SIZES[a], SIZES[a]) for a in SIZES}

    barrier = pltpu.get_barrier_semaphore()
    for ox, oy, oz in NEAR:
        pl.semaphore_signal(barrier, inc=1, device_id=at(ox, oy, oz), device_id_type=MESH)

    loads = [
        pltpu.make_async_copy(a, b, arg_sem.at[i])
        for i, (a, b) in enumerate(
            ((coords_hbm, coords), (polar_hbm, polar), (field_hbm, field), (count_hbm, count), (pairs_hbm, pairs))
        )
    ]
    for load in loads:
        load.start()
    lane, sub = lanes(), subs()
    l32 = lane & 31
    zz = l32 - 3
    group = lane >> 5
    blk = zz >> 3
    valid = (zz >= 0) & (zz < 24)
    dz = 3 - sub

    for load in loads:
        load.wait()
    for b in range(3):
        slot = lane
        mask = (slot[0:1] < count[0, b]).astype(F32)
        packed[b, 0] = jnp.zeros((8, 128), F32)
        packed[b, 1] = jnp.zeros((8, 128), F32)
        for c in range(6):
            packed[b, 0, c : c + 1, :] = field[6 * b + c] * mask
        pol_row = polar[b]
        packed[b, 0, 6:7, :] = pol_row
        s1 = slot[0:1]
        for c, step in enumerate((s1 & 3, (s1 >> 2) & 3, s1 >> 4)):
            site = step.astype(F32) + 0.5
            packed[b, 1, c : c + 1, :] = (coords[3 * b + c] - site * HIGH) - site * LOW
        packed[b, 1, 3:4, :] = mask * lax.rsqrt(pol_row)
    bits = []
    for b in range(3):
        word = jnp.int32(0)
        for k in range(13):
            word = word | (jnp.int32(1) << (pairs[b, 0, k] & 31))
        bits.append(word)
    word = jnp.where(blk <= 0, bits[0], jnp.where(blk == 1, bits[1], bits[2]))
    for x in range(4):
        pick = 16 * (zz & 7) + 4 * group + x
        tile = []
        for t in range(2):
            got = [jnp.take_along_axis(packed[b, t], pick, axis=1) for b in range(3)]
            tile.append(jnp.where(valid, jnp.where(blk == 0, got[0], jnp.where(blk == 1, got[1], got[2])), 0.0))
        code = jnp.where(sub == 7, 14, jnp.maximum(15 + 3 * x + sub - 4, 0))
        flag = (lax.shift_right_logical(word, code) & 1).astype(F32)
        first[x, 0:8, :] = jnp.where((sub >= 4) & valid, flag, tile[1])
        src[x] = jnp.where(sub < 6, tile[0], 0.0)
        rows[x] = jnp.where((sub == 6) & valid, tile[0], 1.0)
        p = row_of(rows, x, slice(6, 7))
        pol[x] = p
        ipol[x] = 1.0 / p
        first[x, 8:16, :] = src[x] * p

    def edge_of(tiles):
        out = jnp.zeros((8, 128), F32)
        for x in range(4):
            top = pltpu.roll(tiles[x], (8 * x - 24) % 128, 1)
            low = pltpu.roll(tiles[x], (8 * x + 1) % 128, 1)
            out = jnp.where((l32 >= 8 * x) & (l32 < 8 * x + 3), top, out)
            out = jnp.where((l32 >= 8 * x + 4) & (l32 < 8 * x + 7), low, out)
        return out

    first_edge[0:8, :] = edge_of([first[x, 0:8, :] for x in range(4)])
    first_edge[8:16, :] = edge_of([first[x, 8:16, :] for x in range(4)])

    pl.semaphore_wait(barrier, len(NEAR))

    def copy(phase, n, incoming):
        ox, oy, oz = n if not incoming else tuple(-v for v in n)
        back = (-ox, -oy, -oz)
        count_rows = 14 if phase == 0 else 6
        if oz == 0:
            lo, hi = (1, 4) if ox == 1 else (0, 3) if ox == -1 else (0, 4)
            if phase == 0:
                s, d = first, in_first.at[FLAT_ID[back]]
            else:
                s, d = vec.at[phase - 1], in_vec.at[phase - 1, FLAT_ID[back]]
            s, d = s.at[lo:hi, 0:count_rows, :], d.at[lo:hi, 0:count_rows, :]
        else:
            if phase == 0:
                s, d = first_edge, in_first_edge.at[EDGE_ID[back]]
            else:
                s, d = vec_edge.at[phase - 1], in_vec_edge.at[phase - 1, EDGE_ID[back]]
            s, d = s.at[0:count_rows, :], d.at[0:count_rows, :]
        return pltpu.make_async_remote_copy(
            src_ref=s, dst_ref=d,
            send_sem=send_sem.at[phase, NEAR_ID[(ox, oy, oz)]], recv_sem=recv_sem.at[phase, NEAR_ID[back]],
            device_id=at(ox, oy, oz), device_id_type=MESH,
        )

    def send(phase):
        for n in sorted(NEAR, key=lambda n: -sum(map(abs, n))):
            copy(phase, n, False).start()

    def await_from(phase, far, cross):
        for n in NEAR:
            if (n[0] != 0, n[1] != 0) == (far, cross):
                copy(phase, n, True).wait_recv()

    def ext_tile(phase, r0, ox, oy, x):
        if phase == 0:
            here = first[x, r0 : r0 + 8, :] if (ox, oy) == (0, 0) else in_first[FLAT_ID[(ox, oy, 0)], x, r0 : r0 + 8, :]
            low = in_first_edge[EDGE_ID[(ox, oy, -1)], r0 : r0 + 8, :]
            top = in_first_edge[EDGE_ID[(ox, oy, 1)], r0 : r0 + 8, :]
        else:
            here = vec[phase - 1, x] if (ox, oy) == (0, 0) else in_vec[phase - 1, FLAT_ID[(ox, oy, 0)], x]
            low = in_vec_edge[phase - 1, EDGE_ID[(ox, oy, -1)]]
            top = in_vec_edge[phase - 1, EDGE_ID[(ox, oy, 1)]]
        low = pltpu.roll(low, (-8 * x) % 128, 1)
        top = pltpu.roll(top, (23 - 8 * x) % 128, 1)
        return jnp.where(l32 < 3, low, jnp.where(l32 >= 27, top, here))

    def slide(ref, where, shift):
        return pltpu.roll(row_of(ref, *where), shift % 128, 1, stride=1, stride_axis=0)

    def merge_column(phase, r0, col, cross):
        ox, x = col_home(col)
        if cross:
            above, below = ext_tile(phase, r0, ox, 1, x), ext_tile(phase, r0, ox, -1, x)
            for k in range(4, 7):
                merged[col, k] = jnp.where(group < k - 3, above, below)
        else:
            tile = ext_tile(phase, r0, ox, 0, x)
            merged[col, 0] = pltpu.roll(tile, 64, 1)
            merged[col, 1] = tile

    def slots(cross):
        return (4, 7) if cross else (0, 4)

    def slide_slot(col, k, c):
        turn = k if k < 4 else k - 3
        return slide(merged, (col, min(k, 1) if k < 4 else k, slice(c, c + 1)), -32 * turn - 3 - (64 if k == 0 else 0))

    def spread_dipoles(phase, cols, cross):
        for col in cols:
            merge_column(phase, 8 if phase == 0 else 0, col, cross)
        for col in cols:
            for k in range(*slots(cross)):
                for c in range(6):
                    dip[col, k, c] = slide_slot(col, k, c)

    def steps_y(k):
        if k < 4:
            return jnp.where(group + k < 4, k, k - 4)
        return jnp.where(group + k - 3 < 4, k - 7, k - 3)

    zp = zz + dz
    oz = (lax.shift_right_arithmetic(zp + 8, 3)) - (lax.shift_right_arithmetic(zz + 8, 3))
    lawful = valid & (sub < 7)

    def forward_act(ox, oy):
        x = 0 if ox == 0 else 2 + oy
        k = [row_of(first, x, slice(4 + i, 5 + i)) for i in range(3)]
        return jnp.where(oz == 0, k[1], jnp.where(oz > 0, k[2], k[0]))

    def backward_act(ox, oy):
        x = 0 if ox == 0 else 2 - oy
        ext[0] = ext_tile(0, 0, ox, oy, x)
        k = [slide(ext, (0, slice(4 + i, 5 + i)), -35) for i in range(3)]
        return jnp.where(oz == 0, k[1], jnp.where(oz > 0, k[0], k[2]))

    def self_act():
        ext[0] = ext_tile(0, 0, 0, 0, 0)
        up = row_of(first, 0, slice(7, 8))
        down = slide(ext, (0, slice(7, 8)), -35)
        return jnp.where(oz == 0, 1.0, jnp.where(oz > 0, up, down))

    def acts(ox, cross):
        pick = forward_act if ox > 0 else backward_act
        if not cross:
            act[ox + 1, 0] = jnp.where(lawful, self_act() if ox == 0 else pick(ox, 0), 0.0)
            return
        above = forward_act(0, 1) if ox == 0 else pick(ox, 1)
        below = backward_act(0, -1) if ox == 0 else pick(ox, -1)
        for k in range(4, 7):
            act[ox + 1, k] = jnp.where(lawful, jnp.where(group + k - 3 < 4, below, above), 0.0)

    def spread_geometry(cols, cross):
        for ox in sorted({col_home(c)[0] for c in cols}):
            acts(ox, cross)
        for col in cols:
            merge_column(0, 0, col, cross)
        for col in cols:
            ox, x = col_home(col)
            for k in range(*slots(cross)):
                for c in range(4):
                    tile = slide_slot(col, k, c)
                    if c == 1:
                        tile = tile + SPACING * steps_y(k).astype(F32)
                    if c == 2:
                        tile = tile + SPACING * dz.astype(F32)
                    if c == 3:
                        tile = tile * act[ox + 1, k if cross else 0]
                    geo[col, k, c] = tile

    def tensors(pair_list, base, cross):
        def body(k, carry):
            for i, (x, col) in enumerate(pair_list):
                off_x = col - 3 - x
                dx = geo[col, k, 0] - own_geo[x, 0]
                if off_x:
                    dx = dx + SPACING * off_x
                dy = geo[col, k, 1] - own_geo[x, 1]
                dzz = geo[col, k, 2] - own_geo[x, 2]
                strength = geo[col, k, 3] * own_geo[x, 3]
                if off_x == 0 and not cross:
                    strength = jnp.where((sub == 3) & (k == 0), 0.0, strength)
                r2 = jnp.maximum(dx * dx + dy * dy + dzz * dzz, 1.0)
                ir = lax.rsqrt(r2)
                ir2 = ir * ir
                ir3 = ir * ir2
                u = r2 * (r2 * ir) * strength
                e = jnp.exp(-u)
                l3 = 1.0 - e
                l5 = l3 - u * e
                s = jnp.maximum(1.0 - r2 * (1.0 / CUT2), 0.0)
                si = s * s * ir3
                w3 = si * l3
                w5 = si * l5 * (3.0 * ir2)
                ax, ay, az = w5 * dx, w5 * dy, w5 * dzz
                tens[k, base + i, 0] = ax * dx - w3
                tens[k, base + i, 1] = ax * dy
                tens[k, base + i, 2] = ax * dzz
                tens[k, base + i, 3] = ay * dy - w3
                tens[k, base + i, 4] = ay * dzz
                tens[k, base + i, 5] = az * dzz - w3
            return carry

        lax.fori_loop(*slots(cross), body, 0)

    def apply(pair_list, base, cross, start):
        def body(k, sums):
            sums = list(sums)
            for i, (x, col) in enumerate(pair_list):
                t = [tens[k, base + i, j] for j in range(6)]
                for s in range(2):
                    vx, vy, vz = (dip[col, k, 3 * s + j] for j in range(3))
                    o = 6 * x + 3 * s
                    sums[o] = sums[o] + (t[0] * vx + t[1] * vy + t[2] * vz)
                    sums[o + 1] = sums[o + 1] + (t[1] * vx + t[3] * vy + t[4] * vz)
                    sums[o + 2] = sums[o + 2] + (t[2] * vx + t[4] * vy + t[5] * vz)
            return tuple(sums)

        return lax.fori_loop(*slots(cross), body, start)

    def gather_field(phase):
        sums = tuple(jnp.zeros((8, 128), F32) for _ in range(24))
        for far, cross in ((False, False), (False, True), (True, False), (True, True)):
            cols, pair_list, base = (FAR_COLS, FAR_PAIRS, 16) if far else (OWN_COLS, OWN_PAIRS, 0)
            await_from(phase, far, cross)
            if phase == 0:
                spread_geometry(cols, cross)
                tensors(pair_list, base, cross)
            spread_dipoles(phase, cols, cross)
            if far or cross:
                sums = tuple(acc[i] for i in range(24))
            sums = apply(pair_list, base, cross, sums)
            if not (far and cross):
                for i in range(24):
                    acc[i] = sums[i]
        out = []
        for x in range(4):
            for c in range(6):
                rows[x, c : c + 1, :] = jnp.sum(sums[6 * x + c], axis=0, keepdims=True)
            out.append(jnp.where(sub < 6, rows[x], 0.0))
        return out

    def publish(phase, tiles):
        for x in range(4):
            vec[phase - 1, x] = tiles[x]
        vec_edge[phase - 1] = edge_of(tiles)
        send(phase)

    send(0)
    for x in range(4):
        for c in range(3):
            own_geo[x, c] = row_of(first, x, slice(c, c + 1))
        own_geo[x, 3] = THOLE * row_of(first, x, slice(3, 4))

    d0 = [src[x] * pol[x] for x in range(4)]
    field0 = gather_field(0)
    r0 = [src[x] - (d0[x] * ipol[x] - field0[x]) for x in range(4)]
    p0 = [pol[x] * r0[x] for x in range(4)]
    publish(1, p0)
    field1 = gather_field(1)
    y0 = [p0[x] * ipol[x] - field1[x] for x in range(4)]
    q0 = [pol[x] * y0[x] for x in range(4)]
    publish(2, q0)
    field2 = gather_field(2)
    z0 = [q0[x] * ipol[x] - field2[x] for x in range(4)]

    def dot(a, b):
        t = a[0] * b[0]
        for x in range(1, 4):
            t = t + a[x] * b[x]
        return jnp.sum(t, axis=1, keepdims=True)

    set_of = jnp.where(sub < 3, 0, 1)
    four = [dot(r0, p0), dot(p0, y0), dot(y0, q0), dot(q0, z0)]
    mix = jnp.zeros((8, 128), F32)
    for k in range(4):
        mix = jnp.where((lane >> 4) == 2 * k + set_of, four[k], mix)
    total = jnp.sum(mix, axis=0, keepdims=True)

    def peer(x, z, y, core):
        chip = lax.rem((me["gz"] >> 1) + y % 4, 4)
        return {"gx": lax.rem(me["gx"] + x % 4, 4), "gy": lax.rem(me["gy"] + z % 4, 4),
                "gz": 2 * chip + ((me["gz"] & 1) ^ core)}

    def sum_copy(stage, n, incoming):
        x, z, y, core = n
        if incoming:
            x, z, y = -x % 4, -z % 4, -y % 4
        group = STAGES[stage]
        there, back = group.index((x, z, y, core)), group.index((-x % 4, -z % 4, -y % 4, core))
        return pltpu.make_async_remote_copy(
            src_ref=part.at[stage], dst_ref=in_sum[stage].at[back],
            send_sem=sum_send[stage].at[there], recv_sem=sum_recv[stage].at[back],
            device_id=peer(x, z, y, core), device_id_type=MESH,
        )

    for stage, group in enumerate(STAGES):
        part[stage] = total
        for n in group:
            sum_copy(stage, n, False).start()
        for n in reversed(group):
            sum_copy(stage, n, True).wait_recv()
        lot = [total] + [in_sum[stage][i] for i in range(len(group))]
        while len(lot) > 1:
            lot = [lot[i] + lot[i + 1] if i + 1 < len(lot) else lot[i] for i in range(0, len(lot), 2)]
        total = lot[0]

    wide = jnp.broadcast_to(total, (8, 128))
    rz0, py, yq, qz = (
        jnp.sum(jnp.where(lane == 16 * (2 * k + set_of), wide, 0.0), axis=1, keepdims=True) for k in range(4)
    )
    gamma0 = rz0 / py
    rz1 = rz0 + gamma0 * (gamma0 * yq - 2.0 * py)
    keep = 1.0 + rz1 / rz0
    gamma1 = rz1 / (keep * (keep * py - 2.0 * gamma0 * yq) + gamma0 * gamma0 * qz)
    by_p = jnp.broadcast_to(gamma0 + gamma1 * keep, (8, 128))
    by_q = jnp.broadcast_to(gamma1 * gamma0, (8, 128))
    slot = lane
    for out, parts in ((dip_out, (d0, 1.0, p0, q0)), (res_out, (r0, -1.0, y0, z0))):
        base, sign, along, across = parts
        tile = [base[x] + sign * (by_p * along[x] - by_q * across[x]) for x in range(4)]
        for b in range(3):
            pick = 32 * ((slot >> 2) & 3) + 3 + 8 * b + (slot >> 4)
            got = [jnp.take_along_axis(tile[x], pick, axis=1) for x in range(4)]
            sx = slot & 3
            whole = jnp.where(sx == 0, got[0], jnp.where(sx == 1, got[1], jnp.where(sx == 2, got[2], got[3])))
            for c in range(6):
                out[6 * b + c] = whole[c : c + 1, :]

    for phase in range(3):
        for n in NEAR:
            copy(phase, n, False).wait_send()
    for stage, group in enumerate(STAGES):
        for n in group:
            sum_copy(stage, n, False).wait_send()


def put_out(dipoles, residual, dip_out, res_out, sem):
    copies = [
        pltpu.make_async_copy(a, b, sem.at[i]) for i, (a, b) in enumerate(((dipoles, dip_out), (residual, res_out)))
    ]
    for copy in copies:
        copy.start()
    for copy in copies:
        copy.wait()


def on_device(coords, polar, field, atom_count, pair_list):
    vmem = pl.BlockSpec(memory_space=pltpu.VMEM)
    tile = lambda *n: pltpu.VMEM(tuple(n) + (8, 128), F32)
    dma = lambda *n: pltpu.SemaphoreType.DMA(tuple(n))
    kept = pltpu.VMEM((18, 1, 128), F32)
    dipoles, residual = pl.pallas_call(
        kernel,
        out_shape=(kept, kept),
        in_specs=[pl.BlockSpec(memory_space=pl.ANY)] * 5,
        out_specs=(vmem, vmem),
        scratch_shapes=[
            pltpu.VMEM((9, 1, 128), F32),
            pltpu.VMEM((3, 1, 128), F32),
            pltpu.VMEM((18, 1, 128), F32),
            pltpu.SMEM((1, 3), I32),
            pltpu.SMEM((3, 1, 13), I32),
            dma(5),
            tile(3, 2),
            pltpu.VMEM((4, 16, 128), F32),
            pltpu.VMEM((16, 128), F32),
            tile(2, 4),
            tile(2),
            tile(4),
            tile(4),
            tile(4),
            tile(4, 4),
            pltpu.VMEM((8, 4, 16, 128), F32),
            pltpu.VMEM((18, 16, 128), F32),
            tile(2, 8, 4),
            tile(2, 18),
            tile(1),
            tile(10, 7),
            tile(10, 7, 4),
            tile(3, 7),
            tile(10, 7, 6),
            tile(7, 28, 6),
            tile(24),
            tile(4),
            pltpu.VMEM((len(STAGES), 1, 128), F32),
            dma(3, 26), dma(3, 26),
            *(s for g in STAGES for s in (pltpu.VMEM((len(g), 1, 128), F32), dma(len(g)), dma(len(g)))),
        ],
        compiler_params=pltpu.CompilerParams(collective_id=0, has_side_effects=True),
    )(
        coords.reshape(9, 1, 128), polar.reshape(3, 1, 128), field.reshape(18, 1, 128),
        atom_count.reshape(1, 3), pair_list.reshape(3, 1, 13),
    )
    out = jax.ShapeDtypeStruct((18, 1, 128), F32)
    anywhere = pl.BlockSpec(memory_space=pl.ANY)
    dipoles, residual = pl.pallas_call(
        put_out, out_shape=(out, out), in_specs=[vmem] * 2, out_specs=(anywhere,) * 2, scratch_shapes=[dma(2)],
    )(*(pltpu.with_memory_space_constraint(v, pltpu.VMEM) for v in (dipoles, residual)))
    return dipoles.reshape(field.shape), residual.reshape(field.shape)


def solution(mesh):
    spec = P("gx", "gy", "gz")
    return jax.shard_map(
        on_device, mesh=mesh, in_specs=(spec,) * 5, out_specs=(spec, spec), check_vma=False,
    )
```

```python
import functools

import jax
import jax.numpy as jnp
from jax import lax
from jax.experimental import pallas as pl
from jax.experimental.pallas import tpu as pltpu
from jax.sharding import PartitionSpec as P


F32 = jnp.float32
I32 = jnp.int32
MESH = pl.DeviceIdType.MESH
SPACING = 2.2
HIGH = 2.1875
LOW = 0.0125
CUT2 = 49.0
THOLE = 0.39
SIZES = {"gx": 4, "gy": 4, "gz": 8}

NEAR = [(ox, oy, oz) for ox in (-1, 0, 1) for oy in (-1, 0, 1) for oz in (-1, 0, 1) if (ox, oy, oz) != (0, 0, 0)]
NEAR_ID = {n: i for i, n in enumerate(NEAR)}
FLAT = [n for n in NEAR if n[2] == 0]
FLAT_ID = {n: i for i, n in enumerate(FLAT)}
EDGE = [n for n in NEAR if n[2] != 0]
EDGE_ID = {n: i for i, n in enumerate(EDGE)}


def ring(k):
    return min(k, 4 - k)


def stage_group(xs, zs, ys, cores):
    every = [(x, z, y, c) for x in range(xs) for z in range(zs) for y in range(ys) for c in range(cores)]
    return sorted(every[1:], key=lambda n: -sum(map(ring, n[:3])))


STAGES = [stage_group(1, 1, 1, 2), stage_group(4, 4, 4, 1)]

OWN_COLS = [3, 4, 5, 6]
FAR_COLS = [0, 1, 2, 7, 8, 9]
OWN_PAIRS = [(x, c) for c in OWN_COLS for x in range(4)]
FAR_PAIRS = [(x, c) for c in FAR_COLS for x in range(4) if abs(c - 3 - x) <= 3]


def col_home(col):
    return (-1, col + 1) if col < 3 else (0, col - 3) if col < 7 else (1, col - 7)


def lanes():
    return lax.broadcasted_iota(I32, (8, 128), 1)


def subs():
    return lax.broadcasted_iota(I32, (8, 128), 0)


def row_of(ref, *where):
    return jnp.broadcast_to(ref[where], (8, 128))


def kernel(
    coords_hbm, polar_hbm, field_hbm, count_hbm, pairs_hbm, dip_out, res_out,
    coords, polar, field, count, pairs, arg_sem,
    packed, first, first_edge, vec, vec_edge, src, pol, ipol, own_geo,
    in_first, in_first_edge, in_vec, in_vec_edge, ext, merged, geo, act, dip, tens, acc, rows,
    part, home, send_sem, recv_sem, *sums,
):
    in_sum, sum_send, sum_recv = (sums[i :: 3] for i in range(3))
    me = {a: lax.axis_index(a) for a in SIZES}

    def at(ox, oy, oz):
        off = {"gx": ox, "gy": oy, "gz": oz}
        return {a: lax.rem(me[a] + off[a] % SIZES[a], SIZES[a]) for a in SIZES}

    barrier = pltpu.get_barrier_semaphore()
    for ox, oy, oz in NEAR:
        pl.semaphore_signal(barrier, inc=1, device_id=at(ox, oy, oz), device_id_type=MESH)

    loads = [
        pltpu.make_async_copy(a, b, arg_sem.at[i])
        for i, (a, b) in enumerate(
            ((coords_hbm, coords), (polar_hbm, polar), (field_hbm, field), (count_hbm, count), (pairs_hbm, pairs))
        )
    ]
    for load in loads:
        load.start()
    lane, sub = lanes(), subs()
    l32 = lane & 31
    zz = l32 - 3
    group = lane >> 5
    blk = zz >> 3
    valid = (zz >= 0) & (zz < 24)
    dz = 3 - sub

    for load in loads:
        load.wait()
    for b in range(3):
        slot = lane
        mask = (slot[0:1] < count[0, b]).astype(F32)
        packed[b, 0] = jnp.zeros((8, 128), F32)
        packed[b, 1] = jnp.zeros((8, 128), F32)
        for c in range(6):
            packed[b, 0, c : c + 1, :] = field[6 * b + c] * mask
        pol_row = polar[b]
        packed[b, 0, 6:7, :] = pol_row
        s1 = slot[0:1]
        for c, step in enumerate((s1 & 3, (s1 >> 2) & 3, s1 >> 4)):
            site = step.astype(F32) + 0.5
            packed[b, 1, c : c + 1, :] = (coords[3 * b + c] - site * HIGH) - site * LOW
        packed[b, 1, 3:4, :] = mask * lax.rsqrt(pol_row)
    bits = []
    for b in range(3):
        word = jnp.int32(0)
        for k in range(13):
            word = word | (jnp.int32(1) << (pairs[b, 0, k] & 31))
        bits.append(word)
    word = jnp.where(blk <= 0, bits[0], jnp.where(blk == 1, bits[1], bits[2]))
    for x in range(4):
        pick = 16 * (zz & 7) + 4 * group + x
        tile = []
        for t in range(2):
            got = [jnp.take_along_axis(packed[b, t], pick, axis=1) for b in range(3)]
            tile.append(jnp.where(valid, jnp.where(blk == 0, got[0], jnp.where(blk == 1, got[1], got[2])), 0.0))
        code = jnp.where(sub == 7, 14, jnp.maximum(15 + 3 * x + sub - 4, 0))
        flag = (lax.shift_right_logical(word, code) & 1).astype(F32)
        first[x, 0:8, :] = jnp.where((sub >= 4) & valid, flag, tile[1])
        src[x] = jnp.where(sub < 6, tile[0], 0.0)
        rows[x] = jnp.where((sub == 6) & valid, tile[0], 1.0)
        p = row_of(rows, x, slice(6, 7))
        pol[x] = p
        ipol[x] = 1.0 / p
        first[x, 8:16, :] = src[x] * p

    def edge_of(tiles):
        out = jnp.zeros((8, 128), F32)
        for x in range(4):
            top = pltpu.roll(tiles[x], (8 * x - 24) % 128, 1)
            low = pltpu.roll(tiles[x], (8 * x + 1) % 128, 1)
            out = jnp.where((l32 >= 8 * x) & (l32 < 8 * x + 3), top, out)
            out = jnp.where((l32 >= 8 * x + 4) & (l32 < 8 * x + 7), low, out)
        return out

    first_edge[0:8, :] = edge_of([first[x, 0:8, :] for x in range(4)])
    first_edge[8:16, :] = edge_of([first[x, 8:16, :] for x in range(4)])

    pl.semaphore_wait(barrier, len(NEAR))

    def copy(phase, n, incoming):
        ox, oy, oz = n if not incoming else tuple(-v for v in n)
        back = (-ox, -oy, -oz)
        count_rows = 14 if phase == 0 else 6
        if oz == 0:
            lo, hi = (1, 4) if ox == 1 else (0, 3) if ox == -1 else (0, 4)
            if phase == 0:
                s, d = first, in_first.at[FLAT_ID[back]]
            else:
                s, d = vec.at[phase - 1], in_vec.at[phase - 1, FLAT_ID[back]]
            s, d = s.at[lo:hi, 0:count_rows, :], d.at[lo:hi, 0:count_rows, :]
        else:
            if phase == 0:
                s, d = first_edge, in_first_edge.at[EDGE_ID[back]]
            else:
                s, d = vec_edge.at[phase - 1], in_vec_edge.at[phase - 1, EDGE_ID[back]]
            s, d = s.at[0:count_rows, :], d.at[0:count_rows, :]
        return pltpu.make_async_remote_copy(
            src_ref=s, dst_ref=d,
            send_sem=send_sem.at[phase, NEAR_ID[(ox, oy, oz)]], recv_sem=recv_sem.at[phase, NEAR_ID[back]],
            device_id=at(ox, oy, oz), device_id_type=MESH,
        )

    def send(phase):
        for n in sorted(NEAR, key=lambda n: -sum(map(abs, n))):
            copy(phase, n, False).start()

    def await_from(phase, far, cross):
        for n in NEAR:
            if (n[0] != 0, n[1] != 0) == (far, cross):
                copy(phase, n, True).wait_recv()

    def ext_tile(phase, r0, ox, oy, x):
        if phase == 0:
            here = first[x, r0 : r0 + 8, :] if (ox, oy) == (0, 0) else in_first[FLAT_ID[(ox, oy, 0)], x, r0 : r0 + 8, :]
            low = in_first_edge[EDGE_ID[(ox, oy, -1)], r0 : r0 + 8, :]
            top = in_first_edge[EDGE_ID[(ox, oy, 1)], r0 : r0 + 8, :]
        else:
            here = vec[phase - 1, x] if (ox, oy) == (0, 0) else in_vec[phase - 1, FLAT_ID[(ox, oy, 0)], x]
            low = in_vec_edge[phase - 1, EDGE_ID[(ox, oy, -1)]]
            top = in_vec_edge[phase - 1, EDGE_ID[(ox, oy, 1)]]
        low = pltpu.roll(low, (-8 * x) % 128, 1)
        top = pltpu.roll(top, (23 - 8 * x) % 128, 1)
        return jnp.where(l32 < 3, low, jnp.where(l32 >= 27, top, here))

    def slide(ref, where, shift):
        return pltpu.roll(row_of(ref, *where), shift % 128, 1, stride=1, stride_axis=0)

    def merge_column(phase, r0, col, cross):
        ox, x = col_home(col)
        if cross:
            above, below = ext_tile(phase, r0, ox, 1, x), ext_tile(phase, r0, ox, -1, x)
            for k in range(4, 7):
                merged[col, k] = jnp.where(group < k - 3, above, below)
        else:
            tile = ext_tile(phase, r0, ox, 0, x)
            merged[col, 0] = pltpu.roll(tile, 64, 1)
            merged[col, 1] = tile

    def slots(cross):
        return (4, 7) if cross else (0, 4)

    def slide_slot(col, k, c):
        turn = k if k < 4 else k - 3
        return slide(merged, (col, min(k, 1) if k < 4 else k, slice(c, c + 1)), -32 * turn - 3 - (64 if k == 0 else 0))

    def spread_dipoles(phase, cols, cross):
        for col in cols:
            merge_column(phase, 8 if phase == 0 else 0, col, cross)
        for col in cols:
            for k in range(*slots(cross)):
                for c in range(6):
                    dip[col, k, c] = slide_slot(col, k, c)

    def steps_y(k):
        if k < 4:
            return jnp.where(group + k < 4, k, k - 4)
        return jnp.where(group + k - 3 < 4, k - 7, k - 3)

    zp = zz + dz
    oz = (lax.shift_right_arithmetic(zp + 8, 3)) - (lax.shift_right_arithmetic(zz + 8, 3))
    lawful = valid & (sub < 7)

    def forward_act(ox, oy):
        x = 0 if ox == 0 else 2 + oy
        k = [row_of(first, x, slice(4 + i, 5 + i)) for i in range(3)]
        return jnp.where(oz == 0, k[1], jnp.where(oz > 0, k[2], k[0]))

    def backward_act(ox, oy):
        x = 0 if ox == 0 else 2 - oy
        ext[0] = ext_tile(0, 0, ox, oy, x)
        k = [slide(ext, (0, slice(4 + i, 5 + i)), -35) for i in range(3)]
        return jnp.where(oz == 0, k[1], jnp.where(oz > 0, k[0], k[2]))

    def self_act():
        ext[0] = ext_tile(0, 0, 0, 0, 0)
        up = row_of(first, 0, slice(7, 8))
        down = slide(ext, (0, slice(7, 8)), -35)
        return jnp.where(oz == 0, 1.0, jnp.where(oz > 0, up, down))

    def acts(ox, cross):
        pick = forward_act if ox > 0 else backward_act
        if not cross:
            act[ox + 1, 0] = jnp.where(lawful, self_act() if ox == 0 else pick(ox, 0), 0.0)
            return
        above = forward_act(0, 1) if ox == 0 else pick(ox, 1)
        below = backward_act(0, -1) if ox == 0 else pick(ox, -1)
        for k in range(4, 7):
            act[ox + 1, k] = jnp.where(lawful, jnp.where(group + k - 3 < 4, below, above), 0.0)

    def spread_geometry(cols, cross):
        for ox in sorted({col_home(c)[0] for c in cols}):
            acts(ox, cross)
        for col in cols:
            merge_column(0, 0, col, cross)
        for col in cols:
            ox, x = col_home(col)
            for k in range(*slots(cross)):
                for c in range(4):
                    tile = slide_slot(col, k, c)
                    if c == 1:
                        tile = tile + SPACING * steps_y(k).astype(F32)
                    if c == 2:
                        tile = tile + SPACING * dz.astype(F32)
                    if c == 3:
                        tile = tile * act[ox + 1, k if cross else 0]
                    geo[col, k, c] = tile

    def tensors(pair_list, base, cross):
        def body(k, carry):
            for i, (x, col) in enumerate(pair_list):
                off_x = col - 3 - x
                dx = geo[col, k, 0] - own_geo[x, 0]
                if off_x:
                    dx = dx + SPACING * off_x
                dy = geo[col, k, 1] - own_geo[x, 1]
                dzz = geo[col, k, 2] - own_geo[x, 2]
                strength = geo[col, k, 3] * own_geo[x, 3]
                if off_x == 0 and not cross:
                    strength = jnp.where((sub == 3) & (k == 0), 0.0, strength)
                r2 = jnp.maximum(dx * dx + dy * dy + dzz * dzz, 1.0)
                ir = lax.rsqrt(r2)
                ir2 = ir * ir
                ir3 = ir * ir2
                u = r2 * (r2 * ir) * strength
                e = jnp.exp(-u)
                l3 = 1.0 - e
                l5 = l3 - u * e
                s = jnp.maximum(1.0 - r2 * (1.0 / CUT2), 0.0)
                si = s * s * ir3
                w3 = si * l3
                w5 = si * l5 * (3.0 * ir2)
                ax, ay, az = w5 * dx, w5 * dy, w5 * dzz
                tens[k, base + i, 0] = ax * dx - w3
                tens[k, base + i, 1] = ax * dy
                tens[k, base + i, 2] = ax * dzz
                tens[k, base + i, 3] = ay * dy - w3
                tens[k, base + i, 4] = ay * dzz
                tens[k, base + i, 5] = az * dzz - w3
            return carry

        lax.fori_loop(*slots(cross), body, 0)

    def apply(pair_list, base, cross, start):
        def body(k, sums):
            sums = list(sums)
            for i, (x, col) in enumerate(pair_list):
                t = [tens[k, base + i, j] for j in range(6)]
                for s in range(2):
                    vx, vy, vz = (dip[col, k, 3 * s + j] for j in range(3))
                    o = 6 * x + 3 * s
                    sums[o] = sums[o] + (t[0] * vx + t[1] * vy + t[2] * vz)
                    sums[o + 1] = sums[o + 1] + (t[1] * vx + t[3] * vy + t[4] * vz)
                    sums[o + 2] = sums[o + 2] + (t[2] * vx + t[4] * vy + t[5] * vz)
            return tuple(sums)

        return lax.fori_loop(*slots(cross), body, start)

    def gather_field(phase):
        sums = tuple(jnp.zeros((8, 128), F32) for _ in range(24))
        for far, cross in ((False, False), (False, True), (True, False), (True, True)):
            cols, pair_list, base = (FAR_COLS, FAR_PAIRS, 16) if far else (OWN_COLS, OWN_PAIRS, 0)
            await_from(phase, far, cross)
            if phase == 0:
                spread_geometry(cols, cross)
                tensors(pair_list, base, cross)
            spread_dipoles(phase, cols, cross)
            if far or cross:
                sums = tuple(acc[i] for i in range(24))
            sums = apply(pair_list, base, cross, sums)
            if not (far and cross):
                for i in range(24):
                    acc[i] = sums[i]
        out = []
        for x in range(4):
            for c in range(6):
                rows[x, c : c + 1, :] = jnp.sum(sums[6 * x + c], axis=0, keepdims=True)
            out.append(jnp.where(sub < 6, rows[x], 0.0))
        return out

    def publish(phase, tiles):
        for x in range(4):
            vec[phase - 1, x] = tiles[x]
        vec_edge[phase - 1] = edge_of(tiles)
        send(phase)

    send(0)
    for x in range(4):
        for c in range(3):
            own_geo[x, c] = row_of(first, x, slice(c, c + 1))
        own_geo[x, 3] = THOLE * row_of(first, x, slice(3, 4))

    d0 = [src[x] * pol[x] for x in range(4)]
    field0 = gather_field(0)
    r0 = [src[x] - (d0[x] * ipol[x] - field0[x]) for x in range(4)]
    p0 = [pol[x] * r0[x] for x in range(4)]
    publish(1, p0)
    t0 = gather_field(1)
    s0 = [pol[x] * t0[x] for x in range(4)]
    publish(2, s0)
    set_of = jnp.where(sub < 3, 0, 1)

    def with_dot(mix, k, a, b):
        t = a[0] * b[0]
        for x in range(1, 4):
            t = t + a[x] * b[x]
        return jnp.where((lane >> 4) == 2 * k + set_of, jnp.sum(t, axis=1, keepdims=True), mix)

    mix = jnp.zeros((8, 128), F32)
    for k, (a, b) in enumerate(((r0, p0), (p0, t0), (t0, s0))):
        mix = with_dot(mix, k, a, b)
    field2 = gather_field(2)
    w0 = [s0[x] * ipol[x] - field2[x] for x in range(4)]
    total = jnp.sum(with_dot(mix, 3, s0, w0), axis=0, keepdims=True)

    def in_slot_order(tiles, b):
        pick = 32 * ((lane >> 2) & 3) + 3 + 8 * b + (lane >> 4)
        got = [jnp.take_along_axis(tiles[x], pick, axis=1) for x in range(4)]
        at_x = lane & 3
        return jnp.where(at_x == 0, got[0], jnp.where(at_x == 1, got[1], jnp.where(at_x == 2, got[2], got[3])))

    def peer(x, z, y, core):
        chip = lax.rem((me["gz"] >> 1) + y % 4, 4)
        return {"gx": lax.rem(me["gx"] + x % 4, 4), "gy": lax.rem(me["gy"] + z % 4, 4),
                "gz": 2 * chip + ((me["gz"] & 1) ^ core)}

    def sum_copy(stage, n, incoming):
        x, z, y, core = n
        if incoming:
            x, z, y = -x % 4, -z % 4, -y % 4
        group = STAGES[stage]
        there, back = group.index((x, z, y, core)), group.index((-x % 4, -z % 4, -y % 4, core))
        return pltpu.make_async_remote_copy(
            src_ref=part.at[stage], dst_ref=in_sum[stage].at[back],
            send_sem=sum_send[stage].at[there], recv_sem=sum_recv[stage].at[back],
            device_id=peer(x, z, y, core), device_id_type=MESH,
        )

    for stage, group in enumerate(STAGES):
        part[stage] = total
        for n in group:
            sum_copy(stage, n, False).start()
        if stage == len(STAGES) - 1:
            for b in range(3):
                for i, tiles in enumerate((d0, p0, s0, r0, t0, w0)):
                    home[b, i] = in_slot_order(tiles, b)
        for n in reversed(group):
            sum_copy(stage, n, True).wait_recv()
        lot = [total] + [in_sum[stage][i] for i in range(len(group))]
        while len(lot) > 1:
            lot = [lot[i] + lot[i + 1] if i + 1 < len(lot) else lot[i] for i in range(0, len(lot), 2)]
        total = lot[0]

    wide = jnp.broadcast_to(total, (8, 128))
    rz0, pt, ts, sw = (
        jnp.sum(jnp.where(lane == 16 * (2 * k + set_of), wide, 0.0), axis=1, keepdims=True) for k in range(4)
    )
    over = pt / (rz0 - pt)
    gamma0 = 1.0 + over
    rz1 = over * (over * rz0 - 2.0 * gamma0 * pt) + gamma0 * gamma0 * ts
    keep = rz1 / rz0 - over
    curve = keep * (keep * (rz0 - pt) + 2.0 * gamma0 * (pt - ts)) + gamma0 * gamma0 * sw
    gamma1 = rz1 / curve
    by_p = jnp.broadcast_to(gamma0 + gamma1 * keep, (8, 128))
    by_s = jnp.broadcast_to(gamma1 * gamma0, (8, 128))
    by_r = jnp.broadcast_to(over + gamma1 * keep, (8, 128))
    for b in range(3):
        d, p, s, r, t, w = (home[b, i] for i in range(6))
        for out, slots in ((dip_out, d + by_p * p + by_s * s), (res_out, by_p * t - by_r * r - by_s * w)):
            for c in range(6):
                out[6 * b + c] = slots[c : c + 1, :]

    for phase in range(3):
        for n in NEAR:
            copy(phase, n, False).wait_send()
    for stage, group in enumerate(STAGES):
        for n in group:
            sum_copy(stage, n, False).wait_send()


def put_out(dipoles, residual, dip_out, res_out, sem):
    copies = [
        pltpu.make_async_copy(a, b, sem.at[i]) for i, (a, b) in enumerate(((dipoles, dip_out), (residual, res_out)))
    ]
    for copy in copies:
        copy.start()
    for copy in copies:
        copy.wait()


def on_device(coords, polar, field, atom_count, pair_list):
    vmem = pl.BlockSpec(memory_space=pltpu.VMEM)
    tile = lambda *n: pltpu.VMEM(tuple(n) + (8, 128), F32)
    dma = lambda *n: pltpu.SemaphoreType.DMA(tuple(n))
    kept = pltpu.VMEM((18, 1, 128), F32)
    dipoles, residual = pl.pallas_call(
        kernel,
        out_shape=(kept, kept),
        in_specs=[pl.BlockSpec(memory_space=pl.ANY)] * 5,
        out_specs=(vmem, vmem),
        scratch_shapes=[
            pltpu.VMEM((9, 1, 128), F32),
            pltpu.VMEM((3, 1, 128), F32),
            pltpu.VMEM((18, 1, 128), F32),
            pltpu.SMEM((1, 3), I32),
            pltpu.SMEM((3, 1, 13), I32),
            dma(5),
            tile(3, 2),
            pltpu.VMEM((4, 16, 128), F32),
            pltpu.VMEM((16, 128), F32),
            tile(2, 4),
            tile(2),
            tile(4),
            tile(4),
            tile(4),
            tile(4, 4),
            pltpu.VMEM((8, 4, 16, 128), F32),
            pltpu.VMEM((18, 16, 128), F32),
            tile(2, 8, 4),
            tile(2, 18),
            tile(1),
            tile(10, 7),
            tile(10, 7, 4),
            tile(3, 7),
            tile(10, 7, 6),
            tile(7, 28, 6),
            tile(24),
            tile(4),
            pltpu.VMEM((len(STAGES), 1, 128), F32),
            tile(3, 6),
            dma(3, 26), dma(3, 26),
            *(s for g in STAGES for s in (pltpu.VMEM((len(g), 1, 128), F32), dma(len(g)), dma(len(g)))),
        ],
        compiler_params=pltpu.CompilerParams(collective_id=0, has_side_effects=True),
    )(
        coords.reshape(9, 1, 128), polar.reshape(3, 1, 128), field.reshape(18, 1, 128),
        atom_count.reshape(1, 3), pair_list.reshape(3, 1, 13),
    )
    out = jax.ShapeDtypeStruct((18, 1, 128), F32)
    anywhere = pl.BlockSpec(memory_space=pl.ANY)
    dipoles, residual = pl.pallas_call(
        put_out, out_shape=(out, out), in_specs=[vmem] * 2, out_specs=(anywhere,) * 2, scratch_shapes=[dma(2)],
    )(*(pltpu.with_memory_space_constraint(v, pltpu.VMEM) for v in (dipoles, residual)))
    return dipoles.reshape(field.shape), residual.reshape(field.shape)


def solution(mesh):
    spec = P("gx", "gy", "gz")
    return jax.shard_map(
        on_device, mesh=mesh, in_specs=(spec,) * 5, out_specs=(spec, spec), check_vma=False,
    )
```

```python
import functools

import jax
import jax.numpy as jnp
from jax import lax
from jax.experimental import pallas as pl
from jax.experimental.pallas import tpu as pltpu
from jax.sharding import PartitionSpec as P


F32 = jnp.float32
I32 = jnp.int32
MESH = pl.DeviceIdType.MESH
SPACING = 2.2
HIGH = 2.1875
LOW = 0.0125
CUT2 = 49.0
THOLE = 0.39
SIZES = {"gx": 4, "gy": 4, "gz": 8}

NEAR = [(ox, oy, oz) for ox in (-1, 0, 1) for oy in (-1, 0, 1) for oz in (-1, 0, 1) if (ox, oy, oz) != (0, 0, 0)]
NEAR_ID = {n: i for i, n in enumerate(NEAR)}
FLAT = [n for n in NEAR if n[2] == 0]
FLAT_ID = {n: i for i, n in enumerate(FLAT)}
EDGE = [n for n in NEAR if n[2] != 0]
EDGE_ID = {n: i for i, n in enumerate(EDGE)}


def ring(k):
    return min(k, 4 - k)


def stage_group(xs, zs, ys, cores):
    every = [(x, z, y, c) for x in range(xs) for z in range(zs) for y in range(ys) for c in range(cores)]
    return sorted(every[1:], key=lambda n: -sum(map(ring, n[:3])))


STAGES = [stage_group(1, 1, 1, 2), stage_group(4, 4, 4, 1)]

OWN_COLS = [3, 4, 5, 6]
FAR_COLS = [0, 1, 2, 7, 8, 9]
OWN_PAIRS = [(x, c) for c in OWN_COLS for x in range(4)]
FAR_PAIRS = [(x, c) for c in FAR_COLS for x in range(4) if abs(c - 3 - x) <= 3]


def col_home(col):
    return (-1, col + 1) if col < 3 else (0, col - 3) if col < 7 else (1, col - 7)


def lanes():
    return lax.broadcasted_iota(I32, (8, 128), 1)


def subs():
    return lax.broadcasted_iota(I32, (8, 128), 0)


def row_of(ref, *where):
    return jnp.broadcast_to(ref[where], (8, 128))


def kernel(
    coords_hbm, polar_hbm, field_hbm, count_hbm, pairs_hbm, dip_out, res_out,
    coords, polar, field, count, pairs, arg_sem,
    packed, first, first_edge, vec, vec_edge, src, pol, ipol, own_geo,
    in_first, in_first_edge, in_vec, in_vec_edge, ext, merged, geo, act, dip, tens, acc, rows,
    part, home, send_sem, recv_sem, *sums,
):
    in_sum, sum_send, sum_recv = (sums[i :: 3] for i in range(3))
    me = {a: lax.axis_index(a) for a in SIZES}

    def at(ox, oy, oz):
        off = {"gx": ox, "gy": oy, "gz": oz}
        return {a: lax.rem(me[a] + off[a] % SIZES[a], SIZES[a]) for a in SIZES}

    barrier = pltpu.get_barrier_semaphore()
    for ox, oy, oz in NEAR:
        pl.semaphore_signal(barrier, inc=1, device_id=at(ox, oy, oz), device_id_type=MESH)

    loads = [
        pltpu.make_async_copy(a, b, arg_sem.at[i])
        for i, (a, b) in enumerate(
            ((coords_hbm, coords), (polar_hbm, polar), (field_hbm, field), (count_hbm, count), (pairs_hbm, pairs))
        )
    ]
    for load in loads:
        load.start()
    lane, sub = lanes(), subs()
    l32 = lane & 31
    zz = l32 - 3
    group = lane >> 5
    blk = zz >> 3
    valid = (zz >= 0) & (zz < 24)
    dz = 3 - sub

    for load in loads:
        load.wait()
    for b in range(3):
        slot = lane
        mask = (slot[0:1] < count[0, b]).astype(F32)
        packed[b, 0] = jnp.zeros((8, 128), F32)
        packed[b, 1] = jnp.zeros((8, 128), F32)
        for c in range(6):
            packed[b, 0, c : c + 1, :] = field[6 * b + c] * mask
        pol_row = polar[b]
        packed[b, 0, 6:7, :] = pol_row
        s1 = slot[0:1]
        for c, step in enumerate((s1 & 3, (s1 >> 2) & 3, s1 >> 4)):
            site = step.astype(F32) + 0.5
            packed[b, 1, c : c + 1, :] = (coords[3 * b + c] - site * HIGH) - site * LOW
        packed[b, 1, 3:4, :] = mask * lax.rsqrt(pol_row)
    bits = []
    for b in range(3):
        word = jnp.int32(0)
        for k in range(13):
            word = word | (jnp.int32(1) << (pairs[b, 0, k] & 31))
        bits.append(word)
    word = jnp.where(blk <= 0, bits[0], jnp.where(blk == 1, bits[1], bits[2]))
    for x in range(4):
        pick = 16 * (zz & 7) + 4 * group + x
        tile = []
        for t in range(2):
            got = [jnp.take_along_axis(packed[b, t], pick, axis=1) for b in range(3)]
            tile.append(jnp.where(valid, jnp.where(blk == 0, got[0], jnp.where(blk == 1, got[1], got[2])), 0.0))
        code = jnp.where(sub == 7, 14, jnp.maximum(15 + 3 * x + sub - 4, 0))
        flag = (lax.shift_right_logical(word, code) & 1).astype(F32)
        first[x, 0:8, :] = jnp.where((sub >= 4) & valid, flag, tile[1])
        src[x] = jnp.where(sub < 6, tile[0], 0.0)
        rows[x] = jnp.where((sub == 6) & valid, tile[0], 1.0)
        p = row_of(rows, x, slice(6, 7))
        pol[x] = p
        ipol[x] = 1.0 / p
        first[x, 8:16, :] = src[x] * p

    def edge_of(tiles):
        out = jnp.zeros((8, 128), F32)
        for x in range(4):
            top = pltpu.roll(tiles[x], (8 * x - 24) % 128, 1)
            low = pltpu.roll(tiles[x], (8 * x + 1) % 128, 1)
            out = jnp.where((l32 >= 8 * x) & (l32 < 8 * x + 3), top, out)
            out = jnp.where((l32 >= 8 * x + 4) & (l32 < 8 * x + 7), low, out)
        return out

    first_edge[0:8, :] = edge_of([first[x, 0:8, :] for x in range(4)])
    first_edge[8:16, :] = edge_of([first[x, 8:16, :] for x in range(4)])

    pl.semaphore_wait(barrier, len(NEAR))

    def copy(phase, n, incoming):
        ox, oy, oz = n if not incoming else tuple(-v for v in n)
        back = (-ox, -oy, -oz)
        count_rows = 14 if phase == 0 else 6
        if oz == 0:
            lo, hi = (1, 4) if ox == 1 else (0, 3) if ox == -1 else (0, 4)
            if phase == 0:
                s, d = first, in_first.at[FLAT_ID[back]]
            else:
                s, d = vec.at[phase - 1], in_vec.at[phase - 1, FLAT_ID[back]]
            s, d = s.at[lo:hi, 0:count_rows, :], d.at[lo:hi, 0:count_rows, :]
        else:
            if phase == 0:
                s, d = first_edge, in_first_edge.at[EDGE_ID[back]]
            else:
                s, d = vec_edge.at[phase - 1], in_vec_edge.at[phase - 1, EDGE_ID[back]]
            s, d = s.at[0:count_rows, :], d.at[0:count_rows, :]
        return pltpu.make_async_remote_copy(
            src_ref=s, dst_ref=d,
            send_sem=send_sem.at[phase, NEAR_ID[(ox, oy, oz)]], recv_sem=recv_sem.at[phase, NEAR_ID[back]],
            device_id=at(ox, oy, oz), device_id_type=MESH,
        )

    def send(phase):
        for n in sorted(NEAR, key=lambda n: -sum(map(abs, n))):
            copy(phase, n, False).start()

    def await_from(phase, far, cross):
        for n in NEAR:
            if (n[0] != 0, n[1] != 0) == (far, cross):
                copy(phase, n, True).wait_recv()

    def ext_tile(phase, r0, ox, oy, x):
        if phase == 0:
            here = first[x, r0 : r0 + 8, :] if (ox, oy) == (0, 0) else in_first[FLAT_ID[(ox, oy, 0)], x, r0 : r0 + 8, :]
            low = in_first_edge[EDGE_ID[(ox, oy, -1)], r0 : r0 + 8, :]
            top = in_first_edge[EDGE_ID[(ox, oy, 1)], r0 : r0 + 8, :]
        else:
            here = vec[phase - 1, x] if (ox, oy) == (0, 0) else in_vec[phase - 1, FLAT_ID[(ox, oy, 0)], x]
            low = in_vec_edge[phase - 1, EDGE_ID[(ox, oy, -1)]]
            top = in_vec_edge[phase - 1, EDGE_ID[(ox, oy, 1)]]
        low = pltpu.roll(low, (-8 * x) % 128, 1)
        top = pltpu.roll(top, (23 - 8 * x) % 128, 1)
        return jnp.where(l32 < 3, low, jnp.where(l32 >= 27, top, here))

    def slide(ref, where, shift):
        return pltpu.roll(row_of(ref, *where), shift % 128, 1, stride=1, stride_axis=0)

    def merge_column(phase, r0, col, cross):
        ox, x = col_home(col)
        if cross:
            above, below = ext_tile(phase, r0, ox, 1, x), ext_tile(phase, r0, ox, -1, x)
            for k in range(4, 7):
                merged[col, k] = jnp.where(group < k - 3, above, below)
        else:
            tile = ext_tile(phase, r0, ox, 0, x)
            merged[col, 0] = pltpu.roll(tile, 64, 1)
            merged[col, 1] = tile

    def slots(cross):
        return (4, 7) if cross else (0, 4)

    def slide_slot(col, k, c):
        turn = k if k < 4 else k - 3
        return slide(merged, (col, min(k, 1) if k < 4 else k, slice(c, c + 1)), -32 * turn - 3 - (64 if k == 0 else 0))

    def spread_dipoles(phase, cols, cross):
        for col in cols:
            merge_column(phase, 8 if phase == 0 else 0, col, cross)
        for col in cols:
            for k in range(*slots(cross)):
                for c in range(6):
                    dip[col, k, c] = slide_slot(col, k, c)

    def steps_y(k):
        if k < 4:
            return jnp.where(group + k < 4, k, k - 4)
        return jnp.where(group + k - 3 < 4, k - 7, k - 3)

    zp = zz + dz
    oz = (lax.shift_right_arithmetic(zp + 8, 3)) - (lax.shift_right_arithmetic(zz + 8, 3))
    lawful = valid & (sub < 7)

    def forward_act(ox, oy):
        x = 0 if ox == 0 else 2 + oy
        k = [row_of(first, x, slice(4 + i, 5 + i)) for i in range(3)]
        return jnp.where(oz == 0, k[1], jnp.where(oz > 0, k[2], k[0]))

    def backward_act(ox, oy):
        x = 0 if ox == 0 else 2 - oy
        ext[0] = ext_tile(0, 0, ox, oy, x)
        k = [slide(ext, (0, slice(4 + i, 5 + i)), -35) for i in range(3)]
        return jnp.where(oz == 0, k[1], jnp.where(oz > 0, k[0], k[2]))

    def self_act():
        ext[0] = ext_tile(0, 0, 0, 0, 0)
        up = row_of(first, 0, slice(7, 8))
        down = slide(ext, (0, slice(7, 8)), -35)
        return jnp.where(oz == 0, 1.0, jnp.where(oz > 0, up, down))

    def acts(ox, cross):
        pick = forward_act if ox > 0 else backward_act
        if not cross:
            act[ox + 1, 0] = jnp.where(lawful, self_act() if ox == 0 else pick(ox, 0), 0.0)
            return
        above = forward_act(0, 1) if ox == 0 else pick(ox, 1)
        below = backward_act(0, -1) if ox == 0 else pick(ox, -1)
        for k in range(4, 7):
            act[ox + 1, k] = jnp.where(lawful, jnp.where(group + k - 3 < 4, below, above), 0.0)

    def spread_geometry(cols, cross):
        for ox in sorted({col_home(c)[0] for c in cols}):
            acts(ox, cross)
        for col in cols:
            merge_column(0, 0, col, cross)
        for col in cols:
            ox, x = col_home(col)
            for k in range(*slots(cross)):
                for c in range(4):
                    tile = slide_slot(col, k, c)
                    if c == 1:
                        tile = tile + SPACING * steps_y(k).astype(F32)
                    if c == 2:
                        tile = tile + SPACING * dz.astype(F32)
                    if c == 3:
                        tile = tile * act[ox + 1, k if cross else 0]
                    geo[col, k, c] = tile

    def tensors(pair_list, base, cross):
        def body(k, carry):
            for i, (x, col) in enumerate(pair_list):
                off_x = col - 3 - x
                dx = geo[col, k, 0] - own_geo[x, 0]
                if off_x:
                    dx = dx + SPACING * off_x
                dy = geo[col, k, 1] - own_geo[x, 1]
                dzz = geo[col, k, 2] - own_geo[x, 2]
                strength = geo[col, k, 3] * own_geo[x, 3]
                if off_x == 0 and not cross:
                    strength = jnp.where((sub == 3) & (k == 0), 0.0, strength)
                r2 = jnp.maximum(dx * dx + dy * dy + dzz * dzz, 1.0)
                ir = lax.rsqrt(r2)
                ir2 = ir * ir
                ir3 = ir * ir2
                u = r2 * (r2 * ir) * strength
                e = jnp.exp(-u)
                l3 = 1.0 - e
                l5 = l3 - u * e
                s = jnp.maximum(1.0 - r2 * (1.0 / CUT2), 0.0)
                si = s * s * ir3
                w3 = si * l3
                w5 = si * l5 * (3.0 * ir2)
                ax, ay, az = w5 * dx, w5 * dy, w5 * dzz
                tens[k, base + i, 0] = ax * dx - w3
                tens[k, base + i, 1] = ax * dy
                tens[k, base + i, 2] = ax * dzz
                tens[k, base + i, 3] = ay * dy - w3
                tens[k, base + i, 4] = ay * dzz
                tens[k, base + i, 5] = az * dzz - w3
            return carry

        lax.fori_loop(*slots(cross), body, 0, unroll=True)

    def apply(pair_list, base, cross, start):
        def body(k, sums):
            sums = list(sums)
            for i, (x, col) in enumerate(pair_list):
                t = [tens[k, base + i, j] for j in range(6)]
                for s in range(2):
                    vx, vy, vz = (dip[col, k, 3 * s + j] for j in range(3))
                    o = 6 * x + 3 * s
                    sums[o] = sums[o] + (t[0] * vx + t[1] * vy + t[2] * vz)
                    sums[o + 1] = sums[o + 1] + (t[1] * vx + t[3] * vy + t[4] * vz)
                    sums[o + 2] = sums[o + 2] + (t[2] * vx + t[4] * vy + t[5] * vz)
            return tuple(sums)

        return lax.fori_loop(*slots(cross), body, start, unroll=True)

    def gather_field(phase):
        sums = tuple(jnp.zeros((8, 128), F32) for _ in range(24))
        for far, cross in ((False, False), (False, True), (True, False), (True, True)):
            cols, pair_list, base = (FAR_COLS, FAR_PAIRS, 16) if far else (OWN_COLS, OWN_PAIRS, 0)
            await_from(phase, far, cross)
            if phase == 0:
                spread_geometry(cols, cross)
                tensors(pair_list, base, cross)
            spread_dipoles(phase, cols, cross)
            if far or cross:
                sums = tuple(acc[i] for i in range(24))
            sums = apply(pair_list, base, cross, sums)
            if not (far and cross):
                for i in range(24):
                    acc[i] = sums[i]
        out = []
        for x in range(4):
            for c in range(6):
                rows[x, c : c + 1, :] = jnp.sum(sums[6 * x + c], axis=0, keepdims=True)
            out.append(jnp.where(sub < 6, rows[x], 0.0))
        return out

    def publish(phase, tiles):
        for x in range(4):
            vec[phase - 1, x] = tiles[x]
        vec_edge[phase - 1] = edge_of(tiles)
        send(phase)

    send(0)
    for x in range(4):
        for c in range(3):
            own_geo[x, c] = row_of(first, x, slice(c, c + 1))
        own_geo[x, 3] = THOLE * row_of(first, x, slice(3, 4))

    d0 = [src[x] * pol[x] for x in range(4)]
    field0 = gather_field(0)
    r0 = [src[x] - (d0[x] * ipol[x] - field0[x]) for x in range(4)]
    p0 = [pol[x] * r0[x] for x in range(4)]
    publish(1, p0)
    t0 = gather_field(1)
    s0 = [pol[x] * t0[x] for x in range(4)]
    publish(2, s0)
    set_of = jnp.where(sub < 3, 0, 1)

    def with_dot(mix, k, a, b):
        t = a[0] * b[0]
        for x in range(1, 4):
            t = t + a[x] * b[x]
        return jnp.where((lane >> 4) == 2 * k + set_of, jnp.sum(t, axis=1, keepdims=True), mix)

    mix = jnp.zeros((8, 128), F32)
    for k, (a, b) in enumerate(((r0, p0), (p0, t0), (t0, s0))):
        mix = with_dot(mix, k, a, b)
    field2 = gather_field(2)
    w0 = [s0[x] * ipol[x] - field2[x] for x in range(4)]
    total = jnp.sum(with_dot(mix, 3, s0, w0), axis=0, keepdims=True)

    def in_slot_order(tiles, b):
        pick = 32 * ((lane >> 2) & 3) + 3 + 8 * b + (lane >> 4)
        got = [jnp.take_along_axis(tiles[x], pick, axis=1) for x in range(4)]
        at_x = lane & 3
        return jnp.where(at_x == 0, got[0], jnp.where(at_x == 1, got[1], jnp.where(at_x == 2, got[2], got[3])))

    def peer(x, z, y, core):
        chip = lax.rem((me["gz"] >> 1) + y % 4, 4)
        return {"gx": lax.rem(me["gx"] + x % 4, 4), "gy": lax.rem(me["gy"] + z % 4, 4),
                "gz": 2 * chip + ((me["gz"] & 1) ^ core)}

    def sum_copy(stage, n, incoming):
        x, z, y, core = n
        if incoming:
            x, z, y = -x % 4, -z % 4, -y % 4
        group = STAGES[stage]
        there, back = group.index((x, z, y, core)), group.index((-x % 4, -z % 4, -y % 4, core))
        return pltpu.make_async_remote_copy(
            src_ref=part.at[stage], dst_ref=in_sum[stage].at[back],
            send_sem=sum_send[stage].at[there], recv_sem=sum_recv[stage].at[back],
            device_id=peer(x, z, y, core), device_id_type=MESH,
        )

    for stage, group in enumerate(STAGES):
        part[stage] = total
        for n in group:
            sum_copy(stage, n, False).start()
        if stage == len(STAGES) - 1:
            for b in range(3):
                for i, tiles in enumerate((d0, p0, s0, r0, t0, w0)):
                    home[b, i] = in_slot_order(tiles, b)
            for phase in range(3):
                for n in NEAR:
                    copy(phase, n, False).wait_send()
            for done in range(stage + 1):
                for n in STAGES[done]:
                    sum_copy(done, n, False).wait_send()
        for n in reversed(group):
            sum_copy(stage, n, True).wait_recv()
        lot = [total] + [in_sum[stage][i] for i in range(len(group))]
        while len(lot) > 1:
            lot = [lot[i] + lot[i + 1] if i + 1 < len(lot) else lot[i] for i in range(0, len(lot), 2)]
        total = lot[0]

    wide = jnp.broadcast_to(total, (8, 128))
    rz0, pt, ts, sw = (
        jnp.sum(jnp.where(lane == 16 * (2 * k + set_of), wide, 0.0), axis=1, keepdims=True) for k in range(4)
    )
    over = pt / (rz0 - pt)
    gamma0 = 1.0 + over
    rz1 = over * (over * rz0 - 2.0 * gamma0 * pt) + gamma0 * gamma0 * ts
    keep = rz1 / rz0 - over
    curve = keep * (keep * (rz0 - pt) + 2.0 * gamma0 * (pt - ts)) + gamma0 * gamma0 * sw
    gamma1 = rz1 / curve
    by_p = jnp.broadcast_to(gamma0 + gamma1 * keep, (8, 128))
    by_s = jnp.broadcast_to(gamma1 * gamma0, (8, 128))
    by_r = jnp.broadcast_to(over + gamma1 * keep, (8, 128))
    for b in range(3):
        d, p, s, r, t, w = (home[b, i] for i in range(6))
        for out, slots in ((dip_out, d + by_p * p + by_s * s), (res_out, by_p * t - by_r * r - by_s * w)):
            for c in range(6):
                out[6 * b + c] = slots[c : c + 1, :]


def put_out(dipoles, residual, dip_out, res_out, sem):
    copies = [
        pltpu.make_async_copy(a, b, sem.at[i]) for i, (a, b) in enumerate(((dipoles, dip_out), (residual, res_out)))
    ]
    for copy in copies:
        copy.start()
    for copy in copies:
        copy.wait()


def on_device(coords, polar, field, atom_count, pair_list):
    vmem = pl.BlockSpec(memory_space=pltpu.VMEM)
    tile = lambda *n: pltpu.VMEM(tuple(n) + (8, 128), F32)
    dma = lambda *n: pltpu.SemaphoreType.DMA(tuple(n))
    kept = pltpu.VMEM((18, 1, 128), F32)
    dipoles, residual = pl.pallas_call(
        kernel,
        out_shape=(kept, kept),
        in_specs=[pl.BlockSpec(memory_space=pl.ANY)] * 5,
        out_specs=(vmem, vmem),
        scratch_shapes=[
            pltpu.VMEM((9, 1, 128), F32),
            pltpu.VMEM((3, 1, 128), F32),
            pltpu.VMEM((18, 1, 128), F32),
            pltpu.SMEM((1, 3), I32),
            pltpu.SMEM((3, 1, 13), I32),
            dma(5),
            tile(3, 2),
            pltpu.VMEM((4, 16, 128), F32),
            pltpu.VMEM((16, 128), F32),
            tile(2, 4),
            tile(2),
            tile(4),
            tile(4),
            tile(4),
            tile(4, 4),
            pltpu.VMEM((8, 4, 16, 128), F32),
            pltpu.VMEM((18, 16, 128), F32),
            tile(2, 8, 4),
            tile(2, 18),
            tile(1),
            tile(10, 7),
            tile(10, 7, 4),
            tile(3, 7),
            tile(10, 7, 6),
            tile(7, 28, 6),
            tile(24),
            tile(4),
            pltpu.VMEM((len(STAGES), 1, 128), F32),
            tile(3, 6),
            dma(3, 26), dma(3, 26),
            *(s for g in STAGES for s in (pltpu.VMEM((len(g), 1, 128), F32), dma(len(g)), dma(len(g)))),
        ],
        compiler_params=pltpu.CompilerParams(collective_id=0, has_side_effects=True),
    )(
        coords.reshape(9, 1, 128), polar.reshape(3, 1, 128), field.reshape(18, 1, 128),
        atom_count.reshape(1, 3), pair_list.reshape(3, 1, 13),
    )
    out = jax.ShapeDtypeStruct((18, 1, 128), F32)
    anywhere = pl.BlockSpec(memory_space=pl.ANY)
    dipoles, residual = pl.pallas_call(
        put_out, out_shape=(out, out), in_specs=[vmem] * 2, out_specs=(anywhere,) * 2, scratch_shapes=[dma(2)],
    )(*(pltpu.with_memory_space_constraint(v, pltpu.VMEM) for v in (dipoles, residual)))
    return dipoles.reshape(field.shape), residual.reshape(field.shape)


def solution(mesh):
    spec = P("gx", "gy", "gz")
    return jax.shard_map(
        on_device, mesh=mesh, in_specs=(spec,) * 5, out_specs=(spec, spec), check_vma=False,
    )
```

```python
import functools

import jax
import jax.numpy as jnp
from jax import lax
from jax.experimental import pallas as pl
from jax.experimental.pallas import tpu as pltpu
from jax.sharding import PartitionSpec as P


F32 = jnp.float32
I32 = jnp.int32
MESH = pl.DeviceIdType.MESH
SPACING = 2.2
HIGH = 2.1875
LOW = 0.0125
CUT2 = 49.0
THOLE = 0.39
SIZES = {"gx": 4, "gy": 4, "gz": 8}

NEAR = [(ox, oy, oz) for ox in (-1, 0, 1) for oy in (-1, 0, 1) for oz in (-1, 0, 1) if (ox, oy, oz) != (0, 0, 0)]
NEAR_ID = {n: i for i, n in enumerate(NEAR)}
FLAT = [n for n in NEAR if n[2] == 0]
FLAT_ID = {n: i for i, n in enumerate(FLAT)}
EDGE = [n for n in NEAR if n[2] != 0]
EDGE_ID = {n: i for i, n in enumerate(EDGE)}


def ring(k):
    return min(k, 4 - k)


def stage_group(xs, zs, ys, cores):
    every = [(x, z, y, c) for x in range(xs) for z in range(zs) for y in range(ys) for c in range(cores)]
    return sorted(every[1:], key=lambda n: -sum(map(ring, n[:3])))


STAGES = [stage_group(1, 1, 1, 2), stage_group(4, 4, 4, 1)]

OWN_COLS = [3, 4, 5, 6]
FAR_COLS = [0, 1, 2, 7, 8, 9]
OWN_PAIRS = [(x, c) for c in OWN_COLS for x in range(4)]
FAR_PAIRS = [(x, c) for c in FAR_COLS for x in range(4) if abs(c - 3 - x) <= 3]


def col_home(col):
    return (-1, col + 1) if col < 3 else (0, col - 3) if col < 7 else (1, col - 7)


def lanes():
    return lax.broadcasted_iota(I32, (8, 128), 1)


def subs():
    return lax.broadcasted_iota(I32, (8, 128), 0)


def row_of(ref, *where):
    return jnp.broadcast_to(ref[where], (8, 128))


def kernel(
    coords_hbm, polar_hbm, field_hbm, count_hbm, pairs_hbm, dip_out, res_out,
    coords, polar, field, count, pairs, arg_sem,
    packed, first, first_edge, vec, vec_edge, src, pol, ipol, own_geo,
    in_first, in_first_edge, in_vec, in_vec_edge, ext, merged, geo, act, dip, tens, rows,
    part, home, send_sem, recv_sem, *sums,
):
    in_sum, sum_send, sum_recv = (sums[i :: 3] for i in range(3))
    me = {a: lax.axis_index(a) for a in SIZES}

    def at(ox, oy, oz):
        off = {"gx": ox, "gy": oy, "gz": oz}
        return {a: lax.rem(me[a] + off[a] % SIZES[a], SIZES[a]) for a in SIZES}

    loads = [
        pltpu.make_async_copy(a, b, arg_sem.at[i])
        for i, (a, b) in enumerate(
            ((coords_hbm, coords), (polar_hbm, polar), (field_hbm, field), (count_hbm, count), (pairs_hbm, pairs))
        )
    ]
    for load in loads:
        load.start()
    barrier = pltpu.get_barrier_semaphore()
    for ox, oy, oz in NEAR:
        pl.semaphore_signal(barrier, inc=1, device_id=at(ox, oy, oz), device_id_type=MESH)

    lane, sub = lanes(), subs()
    l32 = lane & 31
    zz = l32 - 3
    group = lane >> 5
    blk = zz >> 3
    valid = (zz >= 0) & (zz < 24)
    dz = 3 - sub

    for load in loads:
        load.wait()
    for b in range(3):
        slot = lane
        mask = (slot[0:1] < count[0, b]).astype(F32)
        packed[b, 0] = jnp.zeros((8, 128), F32)
        packed[b, 1] = jnp.zeros((8, 128), F32)
        for c in range(6):
            packed[b, 0, c : c + 1, :] = field[6 * b + c] * mask
        pol_row = polar[b]
        packed[b, 0, 6:7, :] = pol_row
        s1 = slot[0:1]
        for c, step in enumerate((s1 & 3, (s1 >> 2) & 3, s1 >> 4)):
            site = step.astype(F32) + 0.5
            packed[b, 1, c : c + 1, :] = (coords[3 * b + c] - site * HIGH) - site * LOW
        packed[b, 1, 3:4, :] = mask * lax.rsqrt(pol_row)
    bits = []
    for b in range(3):
        word = jnp.int32(0)
        for k in range(13):
            word = word | (jnp.int32(1) << (pairs[b, 0, k] & 31))
        bits.append(word)
    word = jnp.where(blk <= 0, bits[0], jnp.where(blk == 1, bits[1], bits[2]))
    for x in range(4):
        pick = 16 * (zz & 7) + 4 * group + x
        tile = []
        for t in range(2):
            got = [jnp.take_along_axis(packed[b, t], pick, axis=1) for b in range(3)]
            tile.append(jnp.where(valid, jnp.where(blk == 0, got[0], jnp.where(blk == 1, got[1], got[2])), 0.0))
        code = jnp.where(sub == 7, 14, jnp.maximum(15 + 3 * x + sub - 4, 0))
        flag = (lax.shift_right_logical(word, code) & 1).astype(F32)
        first[x, 0:8, :] = jnp.where((sub >= 4) & valid, flag, tile[1])
        src[x] = jnp.where(sub < 6, tile[0], 0.0)
        rows[x] = jnp.where((sub == 6) & valid, tile[0], 1.0)
        p = row_of(rows, x, slice(6, 7))
        pol[x] = p
        ipol[x] = 1.0 / p
        first[x, 8:16, :] = src[x] * p

    def edge_of(tiles):
        out = jnp.zeros((8, 128), F32)
        for x in range(4):
            top = pltpu.roll(tiles[x], (8 * x - 24) % 128, 1)
            low = pltpu.roll(tiles[x], (8 * x + 1) % 128, 1)
            out = jnp.where((l32 >= 8 * x) & (l32 < 8 * x + 3), top, out)
            out = jnp.where((l32 >= 8 * x + 4) & (l32 < 8 * x + 7), low, out)
        return out

    first_edge[0:8, :] = edge_of([first[x, 0:8, :] for x in range(4)])
    first_edge[8:16, :] = edge_of([first[x, 8:16, :] for x in range(4)])

    pl.semaphore_wait(barrier, len(NEAR))

    def copy(phase, n, incoming):
        ox, oy, oz = n if not incoming else tuple(-v for v in n)
        back = (-ox, -oy, -oz)
        count_rows = 14 if phase == 0 else 6
        if oz == 0:
            lo, hi = (1, 4) if ox == 1 else (0, 3) if ox == -1 else (0, 4)
            if phase == 0:
                s, d = first, in_first.at[FLAT_ID[back]]
            else:
                s, d = vec.at[phase - 1], in_vec.at[phase - 1, FLAT_ID[back]]
            s, d = s.at[lo:hi, 0:count_rows, :], d.at[lo:hi, 0:count_rows, :]
        else:
            if phase == 0:
                s, d = first_edge, in_first_edge.at[EDGE_ID[back]]
            else:
                s, d = vec_edge.at[phase - 1], in_vec_edge.at[phase - 1, EDGE_ID[back]]
            s, d = s.at[0:count_rows, :], d.at[0:count_rows, :]
        return pltpu.make_async_remote_copy(
            src_ref=s, dst_ref=d,
            send_sem=send_sem.at[phase, NEAR_ID[(ox, oy, oz)]], recv_sem=recv_sem.at[phase, NEAR_ID[back]],
            device_id=at(ox, oy, oz), device_id_type=MESH,
        )

    def send(phase):
        for n in sorted(NEAR, key=lambda n: -sum(map(abs, n))):
            copy(phase, n, False).start()

    def await_from(phase, far, cross):
        for n in NEAR:
            if (n[0] != 0, n[1] != 0) == (far, cross):
                copy(phase, n, True).wait_recv()

    def ext_tile(phase, r0, ox, oy, x):
        if phase == 0:
            here = first[x, r0 : r0 + 8, :] if (ox, oy) == (0, 0) else in_first[FLAT_ID[(ox, oy, 0)], x, r0 : r0 + 8, :]
            low = in_first_edge[EDGE_ID[(ox, oy, -1)], r0 : r0 + 8, :]
            top = in_first_edge[EDGE_ID[(ox, oy, 1)], r0 : r0 + 8, :]
        else:
            here = vec[phase - 1, x] if (ox, oy) == (0, 0) else in_vec[phase - 1, FLAT_ID[(ox, oy, 0)], x]
            low = in_vec_edge[phase - 1, EDGE_ID[(ox, oy, -1)]]
            top = in_vec_edge[phase - 1, EDGE_ID[(ox, oy, 1)]]
        low = pltpu.roll(low, (-8 * x) % 128, 1)
        top = pltpu.roll(top, (23 - 8 * x) % 128, 1)
        return jnp.where(l32 < 3, low, jnp.where(l32 >= 27, top, here))

    def slide(ref, where, shift):
        return pltpu.roll(row_of(ref, *where), shift % 128, 1, stride=1, stride_axis=0)

    def merge_column(phase, r0, col, cross):
        ox, x = col_home(col)
        if cross:
            above, below = ext_tile(phase, r0, ox, 1, x), ext_tile(phase, r0, ox, -1, x)
            for k in range(4, 7):
                merged[col, k] = jnp.where(group < k - 3, above, below)
        else:
            tile = ext_tile(phase, r0, ox, 0, x)
            merged[col, 0] = pltpu.roll(tile, 64, 1)
            merged[col, 1] = tile

    def slots(cross):
        return (4, 7) if cross else (0, 4)

    def slide_slot(col, k, c):
        turn = k if k < 4 else k - 3
        return slide(merged, (col, min(k, 1) if k < 4 else k, slice(c, c + 1)), -32 * turn - 3 - (64 if k == 0 else 0))

    def spread_dipoles(phase, cols, cross):
        for col in cols:
            merge_column(phase, 8 if phase == 0 else 0, col, cross)
        for col in cols:
            for k in range(*slots(cross)):
                for c in range(6):
                    dip[col, k, c] = slide_slot(col, k, c)

    def steps_y(k):
        if k < 4:
            return jnp.where(group + k < 4, k, k - 4)
        return jnp.where(group + k - 3 < 4, k - 7, k - 3)

    zp = zz + dz
    oz = (lax.shift_right_arithmetic(zp + 8, 3)) - (lax.shift_right_arithmetic(zz + 8, 3))
    lawful = valid & (sub < 7)

    def forward_act(ox, oy):
        x = 0 if ox == 0 else 2 + oy
        k = [row_of(first, x, slice(4 + i, 5 + i)) for i in range(3)]
        return jnp.where(oz == 0, k[1], jnp.where(oz > 0, k[2], k[0]))

    def backward_act(ox, oy):
        x = 0 if ox == 0 else 2 - oy
        ext[0] = ext_tile(0, 0, ox, oy, x)
        k = [slide(ext, (0, slice(4 + i, 5 + i)), -35) for i in range(3)]
        return jnp.where(oz == 0, k[1], jnp.where(oz > 0, k[0], k[2]))

    def self_act():
        ext[0] = ext_tile(0, 0, 0, 0, 0)
        up = row_of(first, 0, slice(7, 8))
        down = slide(ext, (0, slice(7, 8)), -35)
        return jnp.where(oz == 0, 1.0, jnp.where(oz > 0, up, down))

    def acts(ox, cross):
        pick = forward_act if ox > 0 else backward_act
        if not cross:
            act[ox + 1, 0] = jnp.where(lawful, self_act() if ox == 0 else pick(ox, 0), 0.0)
            return
        above = forward_act(0, 1) if ox == 0 else pick(ox, 1)
        below = backward_act(0, -1) if ox == 0 else pick(ox, -1)
        for k in range(4, 7):
            act[ox + 1, k] = jnp.where(lawful, jnp.where(group + k - 3 < 4, below, above), 0.0)

    def spread_geometry(cols, cross):
        for ox in sorted({col_home(c)[0] for c in cols}):
            acts(ox, cross)
        for col in cols:
            merge_column(0, 0, col, cross)
        for col in cols:
            ox, x = col_home(col)
            for k in range(*slots(cross)):
                for c in range(4):
                    tile = slide_slot(col, k, c)
                    if c == 1:
                        tile = tile + SPACING * steps_y(k).astype(F32)
                    if c == 2:
                        tile = tile + SPACING * dz.astype(F32)
                    if c == 3:
                        tile = tile * act[ox + 1, k if cross else 0]
                    geo[col, k, c] = tile

    def tensors(pair_list, base, cross):
        def body(k, carry):
            for i, (x, col) in enumerate(pair_list):
                off_x = col - 3 - x
                dx = geo[col, k, 0] - own_geo[x, 0]
                if off_x:
                    dx = dx + SPACING * off_x
                dy = geo[col, k, 1] - own_geo[x, 1]
                dzz = geo[col, k, 2] - own_geo[x, 2]
                strength = geo[col, k, 3] * own_geo[x, 3]
                if off_x == 0 and not cross:
                    strength = jnp.where((sub == 3) & (k == 0), 0.0, strength)
                r2 = jnp.maximum(dx * dx + dy * dy + dzz * dzz, 1.0)
                ir = lax.rsqrt(r2)
                ir2 = ir * ir
                ir3 = ir * ir2
                u = r2 * (r2 * ir) * strength
                e = jnp.exp(-u)
                l3 = 1.0 - e
                l5 = l3 - u * e
                s = jnp.maximum(1.0 - r2 * (1.0 / CUT2), 0.0)
                si = s * s * ir3
                w3 = si * l3
                w5 = si * l5 * (3.0 * ir2)
                ax, ay, az = w5 * dx, w5 * dy, w5 * dzz
                tens[k, base + i, 0] = ax * dx - w3
                tens[k, base + i, 1] = ax * dy
                tens[k, base + i, 2] = ax * dzz
                tens[k, base + i, 3] = ay * dy - w3
                tens[k, base + i, 4] = ay * dzz
                tens[k, base + i, 5] = az * dzz - w3
            return carry

        lax.fori_loop(*slots(cross), body, 0, unroll=True)

    def apply(pair_list, base, cross, start):
        def body(k, sums):
            sums = list(sums)
            for i, (x, col) in enumerate(pair_list):
                t = [tens[k, base + i, j] for j in range(6)]
                for s in range(2):
                    vx, vy, vz = (dip[col, k, 3 * s + j] for j in range(3))
                    o = 6 * x + 3 * s
                    sums[o] = sums[o] + (t[0] * vx + t[1] * vy + t[2] * vz)
                    sums[o + 1] = sums[o + 1] + (t[1] * vx + t[3] * vy + t[4] * vz)
                    sums[o + 2] = sums[o + 2] + (t[2] * vx + t[4] * vy + t[5] * vz)
            return tuple(sums)

        return lax.fori_loop(*slots(cross), body, start, unroll=True)

    def gather_field(phase):
        sums = tuple(jnp.zeros((8, 128), F32) for _ in range(24))
        for far, cross in ((False, False), (False, True), (True, False), (True, True)):
            cols, pair_list, base = (FAR_COLS, FAR_PAIRS, 16) if far else (OWN_COLS, OWN_PAIRS, 0)
            await_from(phase, far, cross)
            if phase == 0:
                spread_geometry(cols, cross)
                tensors(pair_list, base, cross)
            spread_dipoles(phase, cols, cross)
            sums = apply(pair_list, base, cross, sums)
        out = []
        for x in range(4):
            for c in range(6):
                rows[x, c : c + 1, :] = jnp.sum(sums[6 * x + c], axis=0, keepdims=True)
            out.append(jnp.where(sub < 6, rows[x], 0.0))
        return out

    def publish(phase, tiles):
        for x in range(4):
            vec[phase - 1, x] = tiles[x]
        vec_edge[phase - 1] = edge_of(tiles)
        send(phase)

    send(0)
    for x in range(4):
        for c in range(3):
            own_geo[x, c] = row_of(first, x, slice(c, c + 1))
        own_geo[x, 3] = THOLE * row_of(first, x, slice(3, 4))

    d0 = [src[x] * pol[x] for x in range(4)]
    field0 = gather_field(0)
    r0 = [src[x] - (d0[x] * ipol[x] - field0[x]) for x in range(4)]
    p0 = [pol[x] * r0[x] for x in range(4)]
    publish(1, p0)
    t0 = gather_field(1)
    s0 = [pol[x] * t0[x] for x in range(4)]
    publish(2, s0)
    set_of = jnp.where(sub < 3, 0, 1)

    def with_dot(mix, k, a, b):
        t = a[0] * b[0]
        for x in range(1, 4):
            t = t + a[x] * b[x]
        return jnp.where((lane >> 4) == 2 * k + set_of, jnp.sum(t, axis=1, keepdims=True), mix)

    mix = jnp.zeros((8, 128), F32)
    for k, (a, b) in enumerate(((r0, p0), (p0, t0), (t0, s0))):
        mix = with_dot(mix, k, a, b)
    field2 = gather_field(2)
    w0 = [s0[x] * ipol[x] - field2[x] for x in range(4)]
    total = jnp.sum(with_dot(mix, 3, s0, w0), axis=0, keepdims=True)

    def in_slot_order(tiles, b):
        pick = 32 * ((lane >> 2) & 3) + 3 + 8 * b + (lane >> 4)
        got = [jnp.take_along_axis(tiles[x], pick, axis=1) for x in range(4)]
        at_x = lane & 3
        return jnp.where(at_x == 0, got[0], jnp.where(at_x == 1, got[1], jnp.where(at_x == 2, got[2], got[3])))

    def peer(x, z, y, core):
        chip = lax.rem((me["gz"] >> 1) + y % 4, 4)
        return {"gx": lax.rem(me["gx"] + x % 4, 4), "gy": lax.rem(me["gy"] + z % 4, 4),
                "gz": 2 * chip + ((me["gz"] & 1) ^ core)}

    def sum_copy(stage, n, incoming):
        x, z, y, core = n
        if incoming:
            x, z, y = -x % 4, -z % 4, -y % 4
        group = STAGES[stage]
        there, back = group.index((x, z, y, core)), group.index((-x % 4, -z % 4, -y % 4, core))
        return pltpu.make_async_remote_copy(
            src_ref=part.at[stage], dst_ref=in_sum[stage].at[back],
            send_sem=sum_send[stage].at[there], recv_sem=sum_recv[stage].at[back],
            device_id=peer(x, z, y, core), device_id_type=MESH,
        )

    for stage, group in enumerate(STAGES):
        part[stage] = total
        for n in group:
            sum_copy(stage, n, False).start()
        if stage == len(STAGES) - 1:
            for b in range(3):
                for i, tiles in enumerate((d0, p0, s0, r0, t0, w0)):
                    home[b, i] = in_slot_order(tiles, b)
            for phase in range(3):
                for n in NEAR:
                    copy(phase, n, False).wait_send()
            for done in range(stage + 1):
                for n in STAGES[done]:
                    sum_copy(done, n, False).wait_send()
        for n in reversed(group):
            sum_copy(stage, n, True).wait_recv()
        lot = [total] + [in_sum[stage][i] for i in range(len(group))]
        while len(lot) > 1:
            lot = [lot[i] + lot[i + 1] if i + 1 < len(lot) else lot[i] for i in range(0, len(lot), 2)]
        total = lot[0]

    wide = jnp.broadcast_to(total, (8, 128))
    rz0, pt, ts, sw = (
        jnp.sum(jnp.where(lane == 16 * (2 * k + set_of), wide, 0.0), axis=1, keepdims=True) for k in range(4)
    )
    over = pt / (rz0 - pt)
    gamma0 = 1.0 + over
    rz1 = over * (over * rz0 - 2.0 * gamma0 * pt) + gamma0 * gamma0 * ts
    keep = rz1 / rz0 - over
    curve = keep * (keep * (rz0 - pt) + 2.0 * gamma0 * (pt - ts)) + gamma0 * gamma0 * sw
    gamma1 = rz1 / curve
    by_p = jnp.broadcast_to(gamma0 + gamma1 * keep, (8, 128))
    by_s = jnp.broadcast_to(gamma1 * gamma0, (8, 128))
    by_r = jnp.broadcast_to(over + gamma1 * keep, (8, 128))
    for b in range(3):
        d, p, s, r, t, w = (home[b, i] for i in range(6))
        for out, slots in ((dip_out, d + by_p * p + by_s * s), (res_out, by_p * t - by_r * r - by_s * w)):
            for c in range(6):
                out[6 * b + c] = slots[c : c + 1, :]


def put_out(dipoles, residual, dip_out, res_out, sem):
    copies = [
        pltpu.make_async_copy(a, b, sem.at[i]) for i, (a, b) in enumerate(((dipoles, dip_out), (residual, res_out)))
    ]
    for copy in copies:
        copy.start()
    for copy in copies:
        copy.wait()


def on_device(coords, polar, field, atom_count, pair_list):
    vmem = pl.BlockSpec(memory_space=pltpu.VMEM)
    tile = lambda *n: pltpu.VMEM(tuple(n) + (8, 128), F32)
    dma = lambda *n: pltpu.SemaphoreType.DMA(tuple(n))
    kept = pltpu.VMEM((18, 1, 128), F32)
    dipoles, residual = pl.pallas_call(
        kernel,
        out_shape=(kept, kept),
        in_specs=[pl.BlockSpec(memory_space=pl.ANY)] * 5,
        out_specs=(vmem, vmem),
        scratch_shapes=[
            pltpu.VMEM((9, 1, 128), F32),
            pltpu.VMEM((3, 1, 128), F32),
            pltpu.VMEM((18, 1, 128), F32),
            pltpu.SMEM((1, 3), I32),
            pltpu.SMEM((3, 1, 13), I32),
            dma(5),
            tile(3, 2),
            pltpu.VMEM((4, 16, 128), F32),
            pltpu.VMEM((16, 128), F32),
            tile(2, 4),
            tile(2),
            tile(4),
            tile(4),
            tile(4),
            tile(4, 4),
            pltpu.VMEM((8, 4, 16, 128), F32),
            pltpu.VMEM((18, 16, 128), F32),
            tile(2, 8, 4),
            tile(2, 18),
            tile(1),
            tile(10, 7),
            tile(10, 7, 4),
            tile(3, 7),
            tile(10, 7, 6),
            tile(7, 28, 6),
            tile(4),
            pltpu.VMEM((len(STAGES), 1, 128), F32),
            tile(3, 6),
            dma(3, 26), dma(3, 26),
            *(s for g in STAGES for s in (pltpu.VMEM((len(g), 1, 128), F32), dma(len(g)), dma(len(g)))),
        ],
        compiler_params=pltpu.CompilerParams(collective_id=0, has_side_effects=True),
    )(
        coords.reshape(9, 1, 128), polar.reshape(3, 1, 128), field.reshape(18, 1, 128),
        atom_count.reshape(1, 3), pair_list.reshape(3, 1, 13),
    )
    out = jax.ShapeDtypeStruct((18, 1, 128), F32)
    anywhere = pl.BlockSpec(memory_space=pl.ANY)
    dipoles, residual = pl.pallas_call(
        put_out, out_shape=(out, out), in_specs=[vmem] * 2, out_specs=(anywhere,) * 2, scratch_shapes=[dma(2)],
    )(*(pltpu.with_memory_space_constraint(v, pltpu.VMEM) for v in (dipoles, residual)))
    return dipoles.reshape(field.shape), residual.reshape(field.shape)


def solution(mesh):
    spec = P("gx", "gy", "gz")
    return jax.shard_map(
        on_device, mesh=mesh, in_specs=(spec,) * 5, out_specs=(spec, spec), check_vma=False,
    )
```

```python
import functools

import jax
import jax.numpy as jnp
from jax import lax
from jax.experimental import pallas as pl
from jax.experimental.pallas import tpu as pltpu
from jax.sharding import PartitionSpec as P


F32 = jnp.float32
I32 = jnp.int32
MESH = pl.DeviceIdType.MESH
SPACING = 2.2
HIGH = 2.1875
LOW = 0.0125
CUT2 = 49.0
THOLE = 0.39
SIZES = {"gx": 4, "gy": 4, "gz": 8}

NEAR = [(ox, oy, oz) for ox in (-1, 0, 1) for oy in (-1, 0, 1) for oz in (-1, 0, 1) if (ox, oy, oz) != (0, 0, 0)]
NEAR_ID = {n: i for i, n in enumerate(NEAR)}
FLAT = [n for n in NEAR if n[2] == 0]
FLAT_ID = {n: i for i, n in enumerate(FLAT)}
EDGE = [n for n in NEAR if n[2] != 0]
EDGE_ID = {n: i for i, n in enumerate(EDGE)}


def ring(k):
    return min(k, 4 - k)


def stage_group(xs, zs, ys, cores):
    every = [(x, z, y, c) for x in range(xs) for z in range(zs) for y in range(ys) for c in range(cores)]
    return sorted(every[1:], key=lambda n: -sum(map(ring, n[:3])))


STAGES = [stage_group(1, 1, 1, 2), stage_group(4, 4, 4, 1)]

OWN_COLS = [3, 4, 5, 6]
FAR_COLS = [0, 1, 2, 7, 8, 9]
OWN_PAIRS = [(x, c) for c in OWN_COLS for x in range(4)]
FAR_PAIRS = [(x, c) for c in FAR_COLS for x in range(4) if abs(c - 3 - x) <= 3]


def col_home(col):
    return (-1, col + 1) if col < 3 else (0, col - 3) if col < 7 else (1, col - 7)


def lanes():
    return lax.broadcasted_iota(I32, (8, 128), 1)


def subs():
    return lax.broadcasted_iota(I32, (8, 128), 0)


def row_of(ref, *where):
    return jnp.broadcast_to(ref[where], (8, 128))


def kernel(
    coords_hbm, polar_hbm, field_hbm, count_hbm, pairs_hbm, dip_out, res_out,
    coords, polar, field, count, pairs, arg_sem,
    packed, first, first_edge, vec, vec_edge, src, pol, ipol, own_geo,
    in_first, in_first_edge, in_vec, in_vec_edge, ext, merged, geo, act, dip, tens, acc, rows,
    part, home, send_sem, recv_sem, *sums,
):
    in_sum, sum_send, sum_recv = (sums[i :: 3] for i in range(3))
    me = {a: lax.axis_index(a) for a in SIZES}

    def at(ox, oy, oz):
        off = {"gx": ox, "gy": oy, "gz": oz}
        return {a: lax.rem(me[a] + off[a] % SIZES[a], SIZES[a]) for a in SIZES}

    barrier = pltpu.get_barrier_semaphore()
    for ox, oy, oz in NEAR:
        pl.semaphore_signal(barrier, inc=1, device_id=at(ox, oy, oz), device_id_type=MESH)

    loads = [
        pltpu.make_async_copy(a, b, arg_sem.at[i])
        for i, (a, b) in enumerate(
            ((coords_hbm, coords), (polar_hbm, polar), (field_hbm, field), (count_hbm, count), (pairs_hbm, pairs))
        )
    ]
    for load in loads:
        load.start()
    lane, sub = lanes(), subs()
    l32 = lane & 31
    zz = l32 - 3
    group = lane >> 5
    blk = zz >> 3
    valid = (zz >= 0) & (zz < 24)
    dz = 3 - sub

    for load in loads:
        load.wait()
    for b in range(3):
        slot = lane
        mask = (slot[0:1] < count[0, b]).astype(F32)
        packed[b, 0] = jnp.zeros((8, 128), F32)
        packed[b, 1] = jnp.zeros((8, 128), F32)
        for c in range(6):
            packed[b, 0, c : c + 1, :] = field[6 * b + c] * mask
        pol_row = polar[b]
        packed[b, 0, 6:7, :] = pol_row
        s1 = slot[0:1]
        for c, step in enumerate((s1 & 3, (s1 >> 2) & 3, s1 >> 4)):
            site = step.astype(F32) + 0.5
            packed[b, 1, c : c + 1, :] = (coords[3 * b + c] - site * HIGH) - site * LOW
        packed[b, 1, 3:4, :] = mask * lax.rsqrt(pol_row)
    bits = []
    for b in range(3):
        word = jnp.int32(0)
        for k in range(13):
            word = word | (jnp.int32(1) << (pairs[b, 0, k] & 31))
        bits.append(word)
    word = jnp.where(blk <= 0, bits[0], jnp.where(blk == 1, bits[1], bits[2]))
    for x in range(4):
        pick = 16 * (zz & 7) + 4 * group + x
        tile = []
        for t in range(2):
            got = [jnp.take_along_axis(packed[b, t], pick, axis=1) for b in range(3)]
            tile.append(jnp.where(valid, jnp.where(blk == 0, got[0], jnp.where(blk == 1, got[1], got[2])), 0.0))
        code = jnp.where(sub == 7, 14, jnp.maximum(15 + 3 * x + sub - 4, 0))
        flag = (lax.shift_right_logical(word, code) & 1).astype(F32)
        first[x, 0:8, :] = jnp.where((sub >= 4) & valid, flag, tile[1])
        src[x] = jnp.where(sub < 6, tile[0], 0.0)
        rows[x] = jnp.where((sub == 6) & valid, tile[0], 1.0)
        p = row_of(rows, x, slice(6, 7))
        pol[x] = p
        ipol[x] = 1.0 / p
        first[x, 8:16, :] = src[x] * p

    def edge_of(tiles):
        out = jnp.zeros((8, 128), F32)
        for x in range(4):
            top = pltpu.roll(tiles[x], (8 * x - 24) % 128, 1)
            low = pltpu.roll(tiles[x], (8 * x + 1) % 128, 1)
            out = jnp.where((l32 >= 8 * x) & (l32 < 8 * x + 3), top, out)
            out = jnp.where((l32 >= 8 * x + 4) & (l32 < 8 * x + 7), low, out)
        return out

    first_edge[0:8, :] = edge_of([first[x, 0:8, :] for x in range(4)])
    first_edge[8:16, :] = edge_of([first[x, 8:16, :] for x in range(4)])

    pl.semaphore_wait(barrier, len(NEAR))

    def copy(phase, n, incoming):
        ox, oy, oz = n if not incoming else tuple(-v for v in n)
        back = (-ox, -oy, -oz)
        count_rows = 14 if phase == 0 else 6
        if oz == 0:
            lo, hi = (1, 4) if ox == 1 else (0, 3) if ox == -1 else (0, 4)
            if phase == 0:
                s, d = first, in_first.at[FLAT_ID[back]]
            else:
                s, d = vec.at[phase - 1], in_vec.at[phase - 1, FLAT_ID[back]]
            s, d = s.at[lo:hi, 0:count_rows, :], d.at[lo:hi, 0:count_rows, :]
        else:
            if phase == 0:
                s, d = first_edge, in_first_edge.at[EDGE_ID[back]]
            else:
                s, d = vec_edge.at[phase - 1], in_vec_edge.at[phase - 1, EDGE_ID[back]]
            s, d = s.at[0:count_rows, :], d.at[0:count_rows, :]
        return pltpu.make_async_remote_copy(
            src_ref=s, dst_ref=d,
            send_sem=send_sem.at[phase, NEAR_ID[(ox, oy, oz)]], recv_sem=recv_sem.at[phase, NEAR_ID[back]],
            device_id=at(ox, oy, oz), device_id_type=MESH,
        )

    def send(phase):
        for n in sorted(NEAR, key=lambda n: -sum(map(abs, n))):
            copy(phase, n, False).start()

    def await_from(phase, far, cross):
        for n in NEAR:
            if (n[0] != 0, n[1] != 0) == (far, cross):
                copy(phase, n, True).wait_recv()

    def ext_tile(phase, r0, ox, oy, x):
        if phase == 0:
            here = first[x, r0 : r0 + 8, :] if (ox, oy) == (0, 0) else in_first[FLAT_ID[(ox, oy, 0)], x, r0 : r0 + 8, :]
            low = in_first_edge[EDGE_ID[(ox, oy, -1)], r0 : r0 + 8, :]
            top = in_first_edge[EDGE_ID[(ox, oy, 1)], r0 : r0 + 8, :]
        else:
            here = vec[phase - 1, x] if (ox, oy) == (0, 0) else in_vec[phase - 1, FLAT_ID[(ox, oy, 0)], x]
            low = in_vec_edge[phase - 1, EDGE_ID[(ox, oy, -1)]]
            top = in_vec_edge[phase - 1, EDGE_ID[(ox, oy, 1)]]
        low = pltpu.roll(low, (-8 * x) % 128, 1)
        top = pltpu.roll(top, (23 - 8 * x) % 128, 1)
        return jnp.where(l32 < 3, low, jnp.where(l32 >= 27, top, here))

    def slide(ref, where, shift):
        return pltpu.roll(row_of(ref, *where), shift % 128, 1, stride=1, stride_axis=0)

    def merge_column(phase, r0, col, cross):
        ox, x = col_home(col)
        if cross:
            above, below = ext_tile(phase, r0, ox, 1, x), ext_tile(phase, r0, ox, -1, x)
            for k in range(4, 7):
                merged[r0 // 8 if phase == 0 else 0, col, k] = jnp.where(group < k - 3, above, below)
        else:
            tile = ext_tile(phase, r0, ox, 0, x)
            merged[r0 // 8 if phase == 0 else 0, col, 0] = pltpu.roll(tile, 64, 1)
            merged[r0 // 8 if phase == 0 else 0, col, 1] = tile

    def slots(cross):
        return (4, 7) if cross else (0, 4)

    def slide_slot(which, col, k, c):
        turn = k if k < 4 else k - 3
        return slide(merged, (which, col, min(k, 1) if k < 4 else k, slice(c, c + 1)), -32 * turn - 3 - (64 if k == 0 else 0))

    def spread_dipoles(phase, cols, cross):
        for col in cols:
            merge_column(phase, 8 if phase == 0 else 0, col, cross)
        for k in range(*slots(cross)):
            for col in cols:
                for c in range(6):
                    dip[col, k, c] = slide_slot(1 if phase == 0 else 0, col, k, c)

    def steps_y(k):
        if k < 4:
            return jnp.where(group + k < 4, k, k - 4)
        return jnp.where(group + k - 3 < 4, k - 7, k - 3)

    zp = zz + dz
    oz = (lax.shift_right_arithmetic(zp + 8, 3)) - (lax.shift_right_arithmetic(zz + 8, 3))
    lawful = valid & (sub < 7)

    def forward_act(ox, oy):
        x = 0 if ox == 0 else 2 + oy
        k = [row_of(first, x, slice(4 + i, 5 + i)) for i in range(3)]
        return jnp.where(oz == 0, k[1], jnp.where(oz > 0, k[2], k[0]))

    def backward_act(ox, oy):
        x = 0 if ox == 0 else 2 - oy
        ext[0] = ext_tile(0, 0, ox, oy, x)
        k = [slide(ext, (0, slice(4 + i, 5 + i)), -35) for i in range(3)]
        return jnp.where(oz == 0, k[1], jnp.where(oz > 0, k[0], k[2]))

    def self_act():
        ext[0] = ext_tile(0, 0, 0, 0, 0)
        up = row_of(first, 0, slice(7, 8))
        down = slide(ext, (0, slice(7, 8)), -35)
        return jnp.where(oz == 0, 1.0, jnp.where(oz > 0, up, down))

    def acts(ox, cross):
        pick = forward_act if ox > 0 else backward_act
        if not cross:
            act[ox + 1, 0] = jnp.where(lawful, self_act() if ox == 0 else pick(ox, 0), 0.0)
            return
        above = forward_act(0, 1) if ox == 0 else pick(ox, 1)
        below = backward_act(0, -1) if ox == 0 else pick(ox, -1)
        for k in range(4, 7):
            act[ox + 1, k] = jnp.where(lawful, jnp.where(group + k - 3 < 4, below, above), 0.0)

    def spread_geometry(cols, cross):
        for ox in sorted({col_home(c)[0] for c in cols}):
            acts(ox, cross)
        for col in cols:
            merge_column(0, 0, col, cross)
        for k in range(*slots(cross)):
            for col in cols:
                ox, x = col_home(col)
                for c in range(4):
                    tile = slide_slot(0, col, k, c)
                    if c == 1:
                        tile = tile + SPACING * steps_y(k).astype(F32)
                    if c == 2:
                        tile = tile + SPACING * dz.astype(F32)
                    if c == 3:
                        tile = tile * act[ox + 1, k if cross else 0]
                    geo[col, k, c] = tile

    def tensors(pair_list, base, cross):
        def body(k, carry):
            for i, (x, col) in enumerate(pair_list):
                off_x = col - 3 - x
                dx = geo[col, k, 0] - own_geo[x, 0]
                if off_x:
                    dx = dx + SPACING * off_x
                dy = geo[col, k, 1] - own_geo[x, 1]
                dzz = geo[col, k, 2] - own_geo[x, 2]
                strength = geo[col, k, 3] * own_geo[x, 3]
                if off_x == 0 and not cross:
                    strength = jnp.where((sub == 3) & (k == 0), 0.0, strength)
                r2 = jnp.maximum(dx * dx + dy * dy + dzz * dzz, 1.0)
                ir = lax.rsqrt(r2)
                ir2 = ir * ir
                ir3 = ir * ir2
                u = r2 * (r2 * ir) * strength
                e = jnp.exp(-u)
                l3 = 1.0 - e
                l5 = l3 - u * e
                s = jnp.maximum(1.0 - r2 * (1.0 / CUT2), 0.0)
                si = s * s * ir3
                w3 = si * l3
                w5 = si * l5 * (3.0 * ir2)
                ax, ay, az = w5 * dx, w5 * dy, w5 * dzz
                tens[k, base + i, 0] = ax * dx - w3
                tens[k, base + i, 1] = ax * dy
                tens[k, base + i, 2] = ax * dzz
                tens[k, base + i, 3] = ay * dy - w3
                tens[k, base + i, 4] = ay * dzz
                tens[k, base + i, 5] = az * dzz - w3
            return carry

        lax.fori_loop(*slots(cross), body, 0, unroll=True)

    def apply(pair_list, base, cross, start):
        def body(k, sums):
            sums = list(sums)
            for i, (x, col) in enumerate(pair_list):
                t = [tens[k, base + i, j] for j in range(6)]
                for s in range(2):
                    vx, vy, vz = (dip[col, k, 3 * s + j] for j in range(3))
                    o = 6 * x + 3 * s
                    sums[o] = sums[o] + (t[0] * vx + t[1] * vy + t[2] * vz)
                    sums[o + 1] = sums[o + 1] + (t[1] * vx + t[3] * vy + t[4] * vz)
                    sums[o + 2] = sums[o + 2] + (t[2] * vx + t[4] * vy + t[5] * vz)
            return tuple(sums)

        return lax.fori_loop(*slots(cross), body, start, unroll=True)

    def gather_field(phase):
        sums = tuple(jnp.zeros((8, 128), F32) for _ in range(24))
        for far, cross in ((False, False), (False, True), (True, False), (True, True)):
            cols, pair_list, base = (FAR_COLS, FAR_PAIRS, 16) if far else (OWN_COLS, OWN_PAIRS, 0)
            await_from(phase, far, cross)
            if phase == 0:
                spread_geometry(cols, cross)
            spread_dipoles(phase, cols, cross)
            if phase == 0:
                tensors(pair_list, base, cross)
            if far or cross:
                sums = tuple(acc[i] for i in range(24))
            sums = apply(pair_list, base, cross, sums)
            if not (far and cross):
                for i in range(24):
                    acc[i] = sums[i]
        out = []
        for x in range(4):
            for c in range(6):
                rows[x, c : c + 1, :] = jnp.sum(sums[6 * x + c], axis=0, keepdims=True)
            out.append(jnp.where(sub < 6, rows[x], 0.0))
        return out

    def publish(phase, tiles):
        for x in range(4):
            vec[phase - 1, x] = tiles[x]
        vec_edge[phase - 1] = edge_of(tiles)
        send(phase)

    send(0)
    for x in range(4):
        for c in range(3):
            own_geo[x, c] = row_of(first, x, slice(c, c + 1))
        own_geo[x, 3] = THOLE * row_of(first, x, slice(3, 4))

    d0 = [src[x] * pol[x] for x in range(4)]
    field0 = gather_field(0)
    r0 = [src[x] - (d0[x] * ipol[x] - field0[x]) for x in range(4)]
    p0 = [pol[x] * r0[x] for x in range(4)]
    publish(1, p0)
    t0 = gather_field(1)
    s0 = [pol[x] * t0[x] for x in range(4)]
    publish(2, s0)
    set_of = jnp.where(sub < 3, 0, 1)

    def with_dot(mix, k, a, b):
        t = a[0] * b[0]
        for x in range(1, 4):
            t = t + a[x] * b[x]
        return jnp.where((lane >> 4) == 2 * k + set_of, jnp.sum(t, axis=1, keepdims=True), mix)

    mix = jnp.zeros((8, 128), F32)
    for k, (a, b) in enumerate(((r0, p0), (p0, t0), (t0, s0))):
        mix = with_dot(mix, k, a, b)
    field2 = gather_field(2)
    w0 = [s0[x] * ipol[x] - field2[x] for x in range(4)]
    total = jnp.sum(with_dot(mix, 3, s0, w0), axis=0, keepdims=True)

    def in_slot_order(tiles, b):
        pick = 32 * ((lane >> 2) & 3) + 3 + 8 * b + (lane >> 4)
        got = [jnp.take_along_axis(tiles[x], pick, axis=1) for x in range(4)]
        at_x = lane & 3
        return jnp.where(at_x == 0, got[0], jnp.where(at_x == 1, got[1], jnp.where(at_x == 2, got[2], got[3])))

    def peer(x, z, y, core):
        chip = lax.rem((me["gz"] >> 1) + y % 4, 4)
        return {"gx": lax.rem(me["gx"] + x % 4, 4), "gy": lax.rem(me["gy"] + z % 4, 4),
                "gz": 2 * chip + ((me["gz"] & 1) ^ core)}

    def sum_copy(stage, n, incoming):
        x, z, y, core = n
        if incoming:
            x, z, y = -x % 4, -z % 4, -y % 4
        group = STAGES[stage]
        there, back = group.index((x, z, y, core)), group.index((-x % 4, -z % 4, -y % 4, core))
        return pltpu.make_async_remote_copy(
            src_ref=part.at[stage], dst_ref=in_sum[stage].at[back],
            send_sem=sum_send[stage].at[there], recv_sem=sum_recv[stage].at[back],
            device_id=peer(x, z, y, core), device_id_type=MESH,
        )

    for stage, group in enumerate(STAGES):
        part[stage] = total
        for n in group:
            sum_copy(stage, n, False).start()
        if stage == len(STAGES) - 1:
            for b in range(3):
                for i, tiles in enumerate((d0, p0, s0, r0, t0, w0)):
                    home[b, i] = in_slot_order(tiles, b)
            for phase in range(3):
                for n in NEAR:
                    copy(phase, n, False).wait_send()
            for done in range(stage + 1):
                for n in STAGES[done]:
                    sum_copy(done, n, False).wait_send()
        for n in reversed(group):
            sum_copy(stage, n, True).wait_recv()
        lot = [total] + [in_sum[stage][i] for i in range(len(group))]
        while len(lot) > 1:
            lot = [lot[i] + lot[i + 1] if i + 1 < len(lot) else lot[i] for i in range(0, len(lot), 2)]
        total = lot[0]

    wide = jnp.broadcast_to(total, (8, 128))
    rz0, pt, ts, sw = (
        jnp.sum(jnp.where(lane == 16 * (2 * k + set_of), wide, 0.0), axis=1, keepdims=True) for k in range(4)
    )
    over = pt / (rz0 - pt)
    gamma0 = 1.0 + over
    rz1 = over * (over * rz0 - 2.0 * gamma0 * pt) + gamma0 * gamma0 * ts
    keep = rz1 / rz0 - over
    curve = keep * (keep * (rz0 - pt) + 2.0 * gamma0 * (pt - ts)) + gamma0 * gamma0 * sw
    gamma1 = rz1 / curve
    by_p = jnp.broadcast_to(gamma0 + gamma1 * keep, (8, 128))
    by_s = jnp.broadcast_to(gamma1 * gamma0, (8, 128))
    by_r = jnp.broadcast_to(over + gamma1 * keep, (8, 128))
    for b in range(3):
        d, p, s, r, t, w = (home[b, i] for i in range(6))
        for out, slots in ((dip_out, d + by_p * p + by_s * s), (res_out, by_p * t - by_r * r - by_s * w)):
            for c in range(6):
                out[6 * b + c] = slots[c : c + 1, :]


def put_out(dipoles, residual, dip_out, res_out, sem):
    copies = [
        pltpu.make_async_copy(a, b, sem.at[i]) for i, (a, b) in enumerate(((dipoles, dip_out), (residual, res_out)))
    ]
    for copy in copies:
        copy.start()
    for copy in copies:
        copy.wait()


def on_device(coords, polar, field, atom_count, pair_list):
    vmem = pl.BlockSpec(memory_space=pltpu.VMEM)
    tile = lambda *n: pltpu.VMEM(tuple(n) + (8, 128), F32)
    dma = lambda *n: pltpu.SemaphoreType.DMA(tuple(n))
    kept = pltpu.VMEM((18, 1, 128), F32)
    dipoles, residual = pl.pallas_call(
        kernel,
        out_shape=(kept, kept),
        in_specs=[pl.BlockSpec(memory_space=pl.ANY)] * 5,
        out_specs=(vmem, vmem),
        scratch_shapes=[
            pltpu.VMEM((9, 1, 128), F32),
            pltpu.VMEM((3, 1, 128), F32),
            pltpu.VMEM((18, 1, 128), F32),
            pltpu.SMEM((1, 3), I32),
            pltpu.SMEM((3, 1, 13), I32),
            dma(5),
            tile(3, 2),
            pltpu.VMEM((4, 16, 128), F32),
            pltpu.VMEM((16, 128), F32),
            tile(2, 4),
            tile(2),
            tile(4),
            tile(4),
            tile(4),
            tile(4, 4),
            pltpu.VMEM((8, 4, 16, 128), F32),
            pltpu.VMEM((18, 16, 128), F32),
            tile(2, 8, 4),
            tile(2, 18),
            tile(1),
            tile(2, 10, 7),
            tile(10, 7, 4),
            tile(3, 7),
            tile(10, 7, 6),
            tile(7, 28, 6),
            tile(24),
            tile(4),
            pltpu.VMEM((len(STAGES), 1, 128), F32),
            tile(3, 6),
            dma(3, 26), dma(3, 26),
            *(s for g in STAGES for s in (pltpu.VMEM((len(g), 1, 128), F32), dma(len(g)), dma(len(g)))),
        ],
        compiler_params=pltpu.CompilerParams(collective_id=0, has_side_effects=True),
    )(
        coords.reshape(9, 1, 128), polar.reshape(3, 1, 128), field.reshape(18, 1, 128),
        atom_count.reshape(1, 3), pair_list.reshape(3, 1, 13),
    )
    out = jax.ShapeDtypeStruct((18, 1, 128), F32)
    anywhere = pl.BlockSpec(memory_space=pl.ANY)
    dipoles, residual = pl.pallas_call(
        put_out, out_shape=(out, out), in_specs=[vmem] * 2, out_specs=(anywhere,) * 2, scratch_shapes=[dma(2)],
    )(*(pltpu.with_memory_space_constraint(v, pltpu.VMEM) for v in (dipoles, residual)))
    return dipoles.reshape(field.shape), residual.reshape(field.shape)


def solution(mesh):
    spec = P("gx", "gy", "gz")
    return jax.shard_map(
        on_device, mesh=mesh, in_specs=(spec,) * 5, out_specs=(spec, spec), check_vma=False,
    )
```
